32 devices in a mesh: intra: 4 (over y, x), inter: 8 (over z, core).
Axes of the slice: x: 2, y: 2, z: 4, core: 2. Of those that a mesh axis runs over, the one named last changes fastest.
Arguments:
- acts: bfloat16 [4096, 4096], P(('intra', 'inter')), may hold values from -6 to 6
- grad_out: bfloat16 [4096, 512], P(('intra', 'inter')), may hold values from -6 to 6
- codes: int32 [4096, 512], P('intra'), may hold values from -127 to 127
- scales: float32 [2048], P('intra'), may hold values from 0.0002 to 0.0008
Outputs:
- grad_in: bfloat16 [4096, 4096], P(('intra', 'inter'))
- grad_w: float32 [4096, 512], P(('intra', 'inter'))
The draws below stay inside these ranges and needn't reach their ends.
All inputs are finite; a program needn't handle non-finite values.
Results may differ from the reference program's by a relative error of at most 0.0049.
Values may be sent and summed in bfloat16 or wider, within the bound.
A program may use at most 64 MiB of HBM per device.

```python
import math
import jax
import jax.numpy as jnp
from jax import lax

D = 4096
KV = 512
TOKENS = 4096


def set_ends(entries, stream_key, low, largest):
    dims = entries.shape
    index_at = [jax.random.randint(jax.random.fold_in(stream_key, axis), (), 0, dims[axis]) for axis in range(len(dims))]
    entries = entries.at[tuple(index_at)].set(low)
    longest = dims.index(max(dims))
    index_at[longest] = (index_at[longest] + 1) % dims[longest]
    return entries.at[tuple(index_at)].set(largest)


def with_spikes(drawn, own_key, source, target, shards_of, factor):
    owner, partner = [(jnp.arange(drawn.shape[position]) // (drawn.shape[position] // shards_of)).reshape([-1 if axis == position else 1 for axis in range(drawn.ndim)]) for position in (source, target)]
    chosen = jax.random.permutation(own_key, shards_of)[partner]
    strong = (owner == chosen) | (owner == (partner + shards_of // 2) % shards_of)
    return jnp.where(strong, factor * drawn, drawn)


def steps_of(key, extent, shards, low, high):
    gain = 1.0
    for dim, blocks in shards:
        draws = jax.random.uniform(jax.random.fold_in(jax.random.fold_in(key, 6), dim), (blocks,), jnp.float32, low / len(shards), high / len(shards))
        gain = gain * jnp.repeat(jnp.exp(draws), extent[dim] // blocks).reshape((-1,) + (1,) * (len(extent) - 1 - dim))
    return gain


def normal_values(stream_key, extent, width, limit, split=(), kind=jnp.bfloat16):
    array = jax.random.normal(stream_key, extent, jnp.float32) * width
    if len(split) > 0:
        array = steps_of(stream_key, extent, split, -0.22, 0.18) * array
    return jnp.clip(array, min=-limit, max=limit).astype(kind)


def noise_with(stream_key, shape, width, bound, shards, heavy, held_as=jnp.bfloat16):
    drawn = width * jax.random.normal(stream_key, shape, jnp.float32)
    if shards:
        drawn = drawn * steps_of(stream_key, shape, shards, -0.22, 0.18)
    return jnp.clip(with_spikes(drawn, jax.random.fold_in(stream_key, 3), *heavy), -bound, bound).astype(held_as)


def setup_inputs(seed: int = 0) -> dict:
    key_of = jax.random.split(jax.random.key(seed), 5)
    return {
        "acts": noise_with(key_of[0], (TOKENS, D), 1.0, 6.0, ((0, 32),), (0, 1, 32, 2.75)),
        "grad_out": normal_values(key_of[1], (TOKENS, KV), 1.0, 6.0, ((0, 32),)),
        "codes": set_ends(jax.random.randint(key_of[2], (D, KV), -127, 128), jax.random.fold_in(key_of[2], 1), -127, 127).astype(jnp.int32),
        "scales": jnp.clip(jnp.exp(math.log(0.0008) - 1.3862944 * jax.random.uniform(key_of[3], (D // 2,), jnp.float32) ** steps_of(key_of[3], (D // 2,), ((0, 4),), -0.2, 0.2)), 0.0002, 0.0008),
    }


def reference(acts, grad_out, codes, scales):
    blocks = codes.astype(jnp.float32).reshape(D // 2, 2 * KV) * scales[:, None]
    weight = blocks.reshape(D, KV).astype(jnp.bfloat16)
    grad_in = jnp.dot(grad_out, weight.T, preferred_element_type=jnp.float32).astype(jnp.bfloat16)
    summed = lax.dot_general(acts, grad_out, (((0,), (0,)), ((), ())), preferred_element_type=jnp.float32)
    grad_w = summed * jnp.float32(1.0 / math.sqrt(TOKENS))
    return (grad_in, grad_w)
```

```python
import functools
import math

import jax
import jax.numpy as jnp
from jax import lax
from jax.experimental import pallas as pl
from jax.experimental.pallas import tpu as pltpu
from jax.sharding import PartitionSpec as P

MESH = pl.DeviceIdType.MESH


def flip(index, mask, extent):
    out = 0
    bit = 1
    while bit < extent:
        digit = lax.rem(index // bit, 2)
        out = out + bit * (1 - digit if mask & bit else digit)
        bit *= 2
    return out


def lane_scale(scale_row, half):
    pick = (
        lax.broadcasted_iota(jnp.int32, (half // 2, half), 1) // 2
        == lax.broadcasted_iota(jnp.int32, (half // 2, half), 0)
    ).astype(jnp.float32).astype(jnp.bfloat16)
    rest = jnp.broadcast_to(scale_row, (16, half // 2))
    total = jnp.zeros((16, half), jnp.float32)
    for _ in range(3):
        top = rest.astype(jnp.bfloat16)
        total = total + jnp.dot(top, pick, preferred_element_type=jnp.float32)
        rest = rest - top.astype(jnp.float32)
    return total[0:1]


def kernel(
    ni, nj, acts, go, codes, scales, gin, gw,
    go_all, acts_v, codes_v, scale_v, code_b, code_d, scale_d, ac, pieces, part, rs,
    load_sem, go_send, go_recv, gh_send, gh_recv, fw_send, a_send, a_recv, p_send, p_recv,
    r_send, r_recv, w_send, w_recv, s_send, s_recv, plane_sem, line_sem,
):
    tok, width = acts.shape
    rows = codes.shape[0]
    half = rows // 2
    nz = nj // 2
    blk = rows // nj
    i = lax.axis_index("intra")
    j = lax.axis_index("inter")
    z = j // 2
    c = lax.rem(j, 2)
    oc = 1 - c
    me = 2 * i + c
    peers = {d: flip(i, d, ni) for d in range(ni)}
    near, diag = (1, 2), 3
    dd = peers[diag]
    cores = (c, oc)

    def dev(ii, zz, cc):
        return {"intra": ii, "inter": 2 * zz + cc}

    def rdma(src, dst, s, r, where):
        return pltpu.make_async_remote_copy(
            src_ref=src, dst_ref=dst, send_sem=s, recv_sem=r, device_id=where, device_id_type=MESH
        )

    def arrived(ref, s, r):
        rdma(ref, ref, s, r, dev(i, z, oc)).wait_recv()

    sends = []

    def send(*args):
        cp = rdma(*args)
        cp.start()
        sends.append(cp)

    def go_slot(m):
        return go_all.at[pl.ds(pl.multiple_of(m * tok, tok), tok)]

    def go_half(m, n):
        return go_all.at[pl.ds(pl.multiple_of(m * tok + n * (tok // 2), tok // 2), tok // 2)]

    def ac_slot(h, m):
        return ac.at[h, pl.ds(pl.multiple_of(m * tok, tok), tok)]

    def cols_of(ii, cc):
        return pl.ds(pl.multiple_of(ii * rows + cc * half, half), half)

    def quarter(h):
        return pl.ds(pl.multiple_of(h * blk, blk), blk)

    half_start = pl.multiple_of(c * half, half)
    sc_start = pl.multiple_of(c * (half // 2), half // 2)
    barrier = pltpu.get_barrier_semaphore()
    for d in range(1, ni):
        pl.semaphore_signal(barrier, inc=1, device_id=dev(peers[d], z, 0), device_id_type=MESH)

    @pl.when(c == 1)
    def _():
        pl.semaphore_signal(barrier, inc=1, device_id=dev(i, z, 0), device_id_type=MESH)

    load_go = pltpu.make_async_copy(go, go_slot(me), load_sem.at[0])
    load_go.start()
    load_codes = pltpu.make_async_copy(codes.at[pl.ds(half_start, half)], codes_v, load_sem.at[2])
    load_codes.start()
    load_acts = pltpu.make_async_copy(acts, acts_v, load_sem.at[1])
    load_acts.start()
    load_scale = pltpu.make_async_copy(scales.at[:, pl.ds(sc_start, half // 2)], scale_v, load_sem.at[3])
    load_scale.start()
    for k in range(1, nz):
        pl.semaphore_signal(barrier, inc=1, device_id=dev(i, lax.rem(z + k, nz), 1), device_id_type=MESH)

    load_go.wait()

    @pl.when(c == 0)
    def _():
        pl.semaphore_wait(barrier, 2 * ni - 1)
        pl.semaphore_signal(plane_sem, inc=1, device_id=dev(i, z, 1), device_id_type=MESH)

    @pl.when(c == 1)
    def _():
        pl.semaphore_wait(plane_sem, 1)

    for d in near:
        send(go_slot(me), go_slot(me), go_send.at[d], go_recv.at[me], dev(peers[d], z, c))
    send(go_slot(me), go_slot(me), go_send.at[0], go_recv.at[me], dev(i, z, oc))

    load_codes.wait()
    code_b[...] = codes_v[...].astype(jnp.float32).astype(jnp.bfloat16)
    load_scale.wait()
    send(scale_v, scale_d, s_send, s_recv, dev(dd, z, c))
    row_scale = lane_scale(scale_v[...], half)
    send(code_b.at[quarter(z)], code_d.at[quarter(z)], w_send.at[0], w_recv.at[z], dev(dd, z, c))

    load_acts.wait()
    order = [lax.rem(z + k, nz) for k in range(1, nz)] + [z]
    own = []

    def send_columns(h):
        for d in near + (0, diag):
            for k, cc in enumerate(cores):
                ii = peers[d]
                col = pl.multiple_of(ii * rows + (2 * h + cc) * blk, blk)
                src = acts_v.at[:, pl.ds(col, blk)]
                if d or k:
                    m = 2 * ii + cc
                    send(src, ac_slot(h, me), a_send.at[m, h], a_recv.at[me, h], dev(ii, z, cc))
                else:
                    cp = pltpu.make_async_copy(src, ac_slot(h, me), a_recv.at[me, h])
                    cp.start()
                    own.append(cp)

    send_columns(order[0])

    def wait_go(m):
        arrived(go_slot(m), go_send.at[0], go_recv.at[m])

    for n, d in enumerate(near):
        m = 2 * peers[d] + c
        wait_go(m)
        send(go_half(m, n), go_half(m, n), gh_send.at[n], gh_recv.at[n], dev(peers[diag ^ d], z, c))
        send(go_slot(m), go_slot(m), fw_send.at[d], go_recv.at[m], dev(i, z, oc))
    for h in order[1:]:
        send_columns(h)

    def pieces_of(ii, code, scale):
        pair = go_all[pl.ds(pl.multiple_of(2 * ii * tok, 2 * tok), 2 * tok)]
        out = lax.dot_general(
            pair, code[...], (((1,), (1,)), ((), ())), preferred_element_type=jnp.float32
        )
        return (out * scale).astype(jnp.bfloat16)

    def piece(n, cc):
        return pieces.at[n, pl.ds(pl.multiple_of(cc * tok, tok), tok)]

    for d in near:
        ii = peers[d]
        wait_go(2 * ii + oc)
        pieces[d] = pieces_of(ii, code_b, row_scale)
        for cc in cores:
            m = 2 * ii + cc
            send(piece(d, cc), gin.at[:, cols_of(i, c)], p_send.at[m], p_recv.at[me], dev(ii, z, cc))
    wait_go(2 * i + oc)
    pieces[0] = pieces_of(i, code_b, row_scale)
    send(piece(0, oc), gin.at[:, cols_of(i, c)], p_send.at[2 * i + oc], p_recv.at[me], dev(i, z, oc))
    keep = pltpu.make_async_copy(piece(0, c), gin.at[:, cols_of(i, c)], p_recv.at[me])
    keep.start()

    @pl.when(c == 1)
    def _():
        pl.semaphore_wait(barrier, 2 * (nz - 1))
        pl.semaphore_signal(line_sem, inc=1, device_id=dev(i, z, 0), device_id_type=MESH)

    @pl.when(c == 0)
    def _():
        pl.semaphore_wait(line_sem, 1)

    arrived(code_d.at[quarter(z)], w_send.at[0], w_recv.at[z])
    for k in range(1, nz):
        send(code_d.at[quarter(z)], code_d.at[quarter(z)], w_send.at[k], w_recv.at[z],
             dev(i, lax.rem(z + k, nz), c))

    m = 2 * dd + c
    for n in range(2):
        arrived(go_half(m, n), gh_send.at[n], gh_recv.at[n])
    send(go_slot(m), go_slot(m), fw_send.at[diag], go_recv.at[m], dev(i, z, oc))
    arrived(scale_d, s_send, s_recv)
    far_scale = lane_scale(scale_d[...], half)
    wait_go(2 * dd + oc)

    mine = None
    for n, h in enumerate(order):
        own[n].wait()
        for d in range(ni):
            for k, cc in enumerate(cores):
                if d or k:
                    m = 2 * peers[d] + cc
                    arrived(ac_slot(h, m), a_send.at[m, h], a_recv.at[m, h])
        term = lax.dot_general(
            ac[h], go_all[...], (((0,), (0,)), ((), ())), preferred_element_type=jnp.float32
        )
        if n < nz - 1:
            part[n] = term.astype(jnp.bfloat16)
            send(part.at[n], rs.at[z], r_send.at[n], r_recv.at[z], dev(i, h, c))
        else:
            mine = term

    for k in range(1, nz):
        h = lax.rem(z + k, nz)
        arrived(code_d.at[quarter(h)], w_send.at[k], w_recv.at[h])
    pieces[diag] = pieces_of(i, code_d, far_scale)
    far = gin.at[:, cols_of(dd, c)]
    send(piece(diag, oc), far, p_send.at[2 * dd + c], p_recv.at[2 * dd + c], dev(i, z, oc))
    keep_far = pltpu.make_async_copy(piece(diag, c), far, load_sem.at[0])
    keep_far.start()

    for k in range(1, nz):
        h = lax.rem(z + k, nz)
        arrived(rs.at[h], r_send.at[0], r_recv.at[h])
        mine = mine + rs[h].astype(jnp.float32)
    gw[...] = mine * (1.0 / math.sqrt(tok * ni * nj))

    keep.wait()
    keep_far.wait()
    for d in (0,) + near:
        for k, cc in enumerate(cores):
            if d or k:
                ii = peers[d]
                block = gin.at[:, cols_of(ii, cc)]
                arrived(block, p_send.at[2 * ii + cc], p_recv.at[2 * ii + cc])
    arrived(gin.at[:, cols_of(dd, oc)], p_send.at[2 * dd + oc], p_recv.at[2 * dd + oc])
    for cp in sends:
        cp.wait_send()


def leave(gin, gw, gin_out, gw_out, sem):
    copies = [
        pltpu.make_async_copy(gin, gin_out, sem.at[0]),
        pltpu.make_async_copy(gw, gw_out, sem.at[1]),
    ]
    for cp in copies:
        cp.start()
    for cp in copies:
        cp.wait()


def fused(ni, nj, acts, grad_out, codes, scales):
    tok, width = acts.shape
    kv = grad_out.shape[1]
    rows = codes.shape[0]
    half, nz, blk = rows // 2, nj // 2, rows // nj
    group = 2 * ni
    dma = pltpu.SemaphoreType.DMA
    bf16 = jnp.bfloat16
    anyspace = pl.BlockSpec(memory_space=pl.ANY)
    gin, gw = pl.pallas_call(
        functools.partial(kernel, ni, nj),
        out_shape=(
            pltpu.VMEM((tok, width), bf16),
            pltpu.VMEM((blk, kv), jnp.float32),
        ),
        in_specs=[anyspace] * 4,
        out_specs=(pl.BlockSpec(memory_space=pltpu.VMEM),) * 2,
        scratch_shapes=[
            pltpu.VMEM((group * tok, kv), bf16),
            pltpu.VMEM((tok, width), bf16),
            pltpu.VMEM((half, kv), jnp.int32),
            pltpu.VMEM((1, half // 2), jnp.float32),
            pltpu.VMEM((half, kv), bf16),
            pltpu.VMEM((half, kv), bf16),
            pltpu.VMEM((1, half // 2), jnp.float32),
            pltpu.VMEM((nz, group * tok, blk), bf16),
            pltpu.VMEM((ni, 2 * tok, half), bf16),
            pltpu.VMEM((max(nz - 1, 1), blk, kv), bf16),
            pltpu.VMEM((nz, blk, kv), bf16),
            dma((4,)),
            dma((ni,)), dma((group,)), dma((2,)), dma((2,)), dma((ni,)),
            dma((group, nz)), dma((group, nz)),
            dma((group,)), dma((group,)),
            dma((nz,)), dma((nz,)),
            dma((nz,)), dma((nz,)), dma, dma,
            pltpu.SemaphoreType.REGULAR, pltpu.SemaphoreType.REGULAR,
        ],
        compiler_params=pltpu.CompilerParams(collective_id=0, has_side_effects=True),
    )(acts, grad_out, codes, scales.reshape(1, -1))
    return tuple(pl.pallas_call(
        leave,
        out_shape=(
            jax.ShapeDtypeStruct((tok, width), bf16),
            jax.ShapeDtypeStruct((blk, kv), jnp.float32),
        ),
        in_specs=[anyspace] * 2,
        out_specs=(anyspace,) * 2,
        scratch_shapes=[dma((2,))],
    )(*(pltpu.with_memory_space_constraint(x, pltpu.VMEM) for x in (gin, gw))))


def plain(acts, grad_out, codes, scales):
    rows = codes.shape[0]
    width_kv = codes.shape[1]
    blocks = codes.astype(jnp.float32).reshape(rows // 2, 2 * width_kv) * scales[:, None]
    local_weight = blocks.reshape(rows, width_kv).astype(jnp.bfloat16)
    n_group = lax.axis_size("intra")
    n_cross = lax.axis_size("inter")
    factor = 1.0 / math.sqrt(acts.shape[0] * n_group * n_cross)
    contract = (((0,), (0,)), ((), ()))
    group_cot = lax.all_gather(grad_out, "intra", axis=0, tiled=True)
    columns_owned = lax.all_to_all(acts, "intra", split_axis=1, concat_axis=0, tiled=True)
    grad_w = lax.psum_scatter(
        lax.dot_general(columns_owned, group_cot, contract, preferred_element_type=jnp.float32)
        * factor,
        "inter",
        scatter_dimension=0,
        tiled=True,
    )
    pieces = jnp.dot(group_cot, local_weight.T, preferred_element_type=jnp.float32).astype(
        jnp.bfloat16
    )
    grad_in = lax.all_to_all(pieces, "intra", split_axis=0, concat_axis=1, tiled=True)
    return (grad_in, grad_w)


def solution(mesh):
    ni, nj = mesh.shape["intra"], mesh.shape["inter"]

    def per_device(acts, grad_out, codes, scales):
        rows = codes.shape[0]
        aligned = rows % (nj * 128) == 0 and rows % 512 == 0 and acts.shape[0] % 16 == 0
        if aligned and nj % 2 == 0 and ni == 4 and acts.shape[1] == ni * rows:
            return fused(ni, nj, acts, grad_out, codes, scales)
        return plain(acts, grad_out, codes, scales)

    in_specs = (
        P(("intra", "inter"), None),
        P(("intra", "inter"), None),
        P("intra", None),
        P("intra"),
    )
    out_specs = (P(("intra", "inter"), None), P(("intra", "inter"), None))
    return jax.shard_map(
        per_device, mesh=mesh, in_specs=in_specs, out_specs=out_specs, check_vma=False
    )
```

```python
import functools
import math

import jax
import jax.numpy as jnp
from jax import lax
from jax.experimental import pallas as pl
from jax.experimental.pallas import tpu as pltpu
from jax.sharding import PartitionSpec as P

MESH = pl.DeviceIdType.MESH


def flip(index, mask, extent):
    out = 0
    bit = 1
    while bit < extent:
        digit = lax.rem(index // bit, 2)
        out = out + bit * (1 - digit if mask & bit else digit)
        bit *= 2
    return out


def lane_scale(scale_row, half):
    pick = (
        lax.broadcasted_iota(jnp.int32, (half // 2, half), 1) // 2
        == lax.broadcasted_iota(jnp.int32, (half // 2, half), 0)
    ).astype(jnp.float32).astype(jnp.bfloat16)
    rest = jnp.broadcast_to(scale_row, (16, half // 2))
    total = jnp.zeros((16, half), jnp.float32)
    for _ in range(3):
        top = rest.astype(jnp.bfloat16)
        total = total + jnp.dot(top, pick, preferred_element_type=jnp.float32)
        rest = rest - top.astype(jnp.float32)
    return total[0:1]


def kernel(
    ni, nj, acts, go, codes, scales, gin, gw,
    go_all, acts_v, codes_v, scale_v, code_b, code_d, scale_d, ac, pieces, part, rs, held, ms,
    load_sem, go_send, go_recv, gh_send, gh_recv, fw_send, a_send, a_recv, p_send, p_recv,
    r_send, r_recv, m_recv, w_send, w_recv, s_send, s_recv, plane_sem, line_sem,
):
    tok, width = acts.shape
    rows = codes.shape[0]
    half = rows // 2
    nz = nj // 2
    blk = rows // nj
    i = lax.axis_index("intra")
    j = lax.axis_index("inter")
    z = j // 2
    c = lax.rem(j, 2)
    oc = 1 - c
    me = 2 * i + c
    peers = {d: flip(i, d, ni) for d in range(ni)}
    near, diag = (1, 2), 3
    dd = peers[diag]
    cores = (c, oc)
    pair = z // 2
    inner = lax.rem(z, 2) != pair
    mate = 2 * pair + 1 - lax.rem(z, 2)
    far_outer = 3 * (1 - pair)
    far_inner = 2 - pair
    order = [far_outer, far_inner, mate, z]

    def dev(ii, zz, cc):
        return {"intra": ii, "inter": 2 * zz + cc}

    def rdma(src, dst, s, r, where):
        return pltpu.make_async_remote_copy(
            src_ref=src, dst_ref=dst, send_sem=s, recv_sem=r, device_id=where, device_id_type=MESH
        )

    def arrived(ref, s, r):
        rdma(ref, ref, s, r, dev(i, z, oc)).wait_recv()

    sends = []

    def send(*args):
        cp = rdma(*args)
        cp.start()
        sends.append(cp)

    def go_slot(m):
        return go_all.at[pl.ds(pl.multiple_of(m * tok, tok), tok)]

    def go_half(m, n):
        return go_all.at[pl.ds(pl.multiple_of(m * tok + n * (tok // 2), tok // 2), tok // 2)]

    def ac_slot(h, m):
        return ac.at[h, pl.ds(pl.multiple_of(m * tok, tok), tok)]

    def cols_of(ii, cc):
        return pl.ds(pl.multiple_of(ii * rows + cc * half, half), half)

    def quarter(h):
        return pl.ds(pl.multiple_of(h * blk, blk), blk)

    half_start = pl.multiple_of(c * half, half)
    sc_start = pl.multiple_of(c * (half // 2), half // 2)
    barrier = pltpu.get_barrier_semaphore()
    for d in range(1, ni):
        pl.semaphore_signal(barrier, inc=1, device_id=dev(peers[d], z, 0), device_id_type=MESH)

    @pl.when(c == 1)
    def _():
        pl.semaphore_signal(barrier, inc=1, device_id=dev(i, z, 0), device_id_type=MESH)

    load_go = pltpu.make_async_copy(go, go_slot(me), load_sem.at[0])
    load_go.start()
    load_codes = pltpu.make_async_copy(codes.at[pl.ds(half_start, half)], codes_v, load_sem.at[2])
    load_codes.start()
    load_acts = pltpu.make_async_copy(acts, acts_v, load_sem.at[1])
    load_acts.start()
    load_scale = pltpu.make_async_copy(scales.at[:, pl.ds(sc_start, half // 2)], scale_v, load_sem.at[3])
    load_scale.start()
    for k in range(1, nz):
        pl.semaphore_signal(barrier, inc=1, device_id=dev(i, lax.rem(z + k, nz), 1), device_id_type=MESH)

    load_go.wait()

    @pl.when(c == 0)
    def _():
        pl.semaphore_wait(barrier, 2 * ni - 1)
        pl.semaphore_signal(plane_sem, inc=1, device_id=dev(i, z, 1), device_id_type=MESH)

    @pl.when(c == 1)
    def _():
        pl.semaphore_wait(plane_sem, 1)

    for d in near:
        send(go_slot(me), go_slot(me), go_send.at[d], go_recv.at[me], dev(peers[d], z, c))
    send(go_slot(me), go_slot(me), go_send.at[0], go_recv.at[me], dev(i, z, oc))

    load_codes.wait()
    code_b[...] = codes_v[...].astype(jnp.float32).astype(jnp.bfloat16)
    load_scale.wait()
    send(scale_v, scale_d, s_send, s_recv, dev(dd, z, c))
    row_scale = lane_scale(scale_v[...], half)
    send(code_b.at[quarter(z)], code_d.at[quarter(z)], w_send.at[0], w_recv.at[z], dev(dd, z, c))

    load_acts.wait()
    own = []

    def send_columns(h):
        for d in near + (0, diag):
            for k, cc in enumerate(cores):
                ii = peers[d]
                col = pl.multiple_of(ii * rows + (2 * h + cc) * blk, blk)
                src = acts_v.at[:, pl.ds(col, blk)]
                if d or k:
                    m = 2 * ii + cc
                    send(src, ac_slot(h, me), a_send.at[m, h], a_recv.at[me, h], dev(ii, z, cc))
                else:
                    cp = pltpu.make_async_copy(src, ac_slot(h, me), a_recv.at[me, h])
                    cp.start()
                    own.append(cp)

    def wait_go(m):
        arrived(go_slot(m), go_send.at[0], go_recv.at[m])

    for n, d in enumerate(near):
        m = 2 * peers[d] + c
        wait_go(m)
        send(go_half(m, n), go_half(m, n), gh_send.at[n], gh_recv.at[n], dev(peers[diag ^ d], z, c))
        send(go_slot(m), go_slot(m), fw_send.at[d], go_recv.at[m], dev(i, z, oc))
    for h in order:
        send_columns(h)

    def pieces_of(ii, code, scale):
        pair = go_all[pl.ds(pl.multiple_of(2 * ii * tok, 2 * tok), 2 * tok)]
        out = lax.dot_general(
            pair, code[...], (((1,), (1,)), ((), ())), preferred_element_type=jnp.float32
        )
        return (out * scale).astype(jnp.bfloat16)

    def piece(n, cc):
        return pieces.at[n, pl.ds(pl.multiple_of(cc * tok, tok), tok)]

    for d in near:
        ii = peers[d]
        wait_go(2 * ii + oc)
        pieces[d] = pieces_of(ii, code_b, row_scale)
        for cc in cores:
            m = 2 * ii + cc
            send(piece(d, cc), gin.at[:, cols_of(i, c)], p_send.at[m], p_recv.at[me], dev(ii, z, cc))
    wait_go(2 * i + oc)
    pieces[0] = pieces_of(i, code_b, row_scale)
    send(piece(0, oc), gin.at[:, cols_of(i, c)], p_send.at[2 * i + oc], p_recv.at[me], dev(i, z, oc))
    keep = pltpu.make_async_copy(piece(0, c), gin.at[:, cols_of(i, c)], p_recv.at[me])
    keep.start()

    @pl.when(c == 1)
    def _():
        pl.semaphore_wait(barrier, 2 * (nz - 1))
        pl.semaphore_signal(line_sem, inc=1, device_id=dev(i, z, 0), device_id_type=MESH)

    @pl.when(c == 0)
    def _():
        pl.semaphore_wait(line_sem, 1)

    def hop(n, h, to):
        return rdma(code_d.at[quarter(h)], code_d.at[quarter(h)], w_send.at[n], w_recv.at[h], dev(i, to, c))

    def landed(h):
        arrived(code_d.at[quarter(h)], w_send.at[0], w_recv.at[h])

    to_mate = hop(1, z, mate)
    relays = [hop(2, z, far_inner), hop(3, mate, far_inner), hop(4, far_inner, mate), hop(5, far_outer, mate)]
    landed(z)
    to_mate.start()
    sends.append(to_mate)

    @pl.when(inner)
    def _():
        relays[0].start()

    m = 2 * dd + c
    for n in range(2):
        arrived(go_half(m, n), gh_send.at[n], gh_recv.at[n])
    send(go_slot(m), go_slot(m), fw_send.at[diag], go_recv.at[m], dev(i, z, oc))
    arrived(scale_d, s_send, s_recv)
    far_scale = lane_scale(scale_d[...], half)
    wait_go(2 * dd + oc)

    @pl.when(inner)
    def _():
        landed(mate)
        relays[1].start()
        landed(far_inner)
        relays[2].start()

    def term_of(n):
        h = order[n]
        own[n].wait()
        for d in range(ni):
            for k, cc in enumerate(cores):
                if d or k:
                    m = 2 * peers[d] + cc
                    arrived(ac_slot(h, m), a_send.at[m, h], a_recv.at[m, h])
        return lax.dot_general(
            ac[h], go_all[...], (((0,), (0,)), ((), ())), preferred_element_type=jnp.float32
        )

    def pass_on(n, dst, recv, to):
        return rdma(part.at[n], dst, r_send.at[n], recv, dev(i, to, c))

    to_inner = [pass_on(n, ms.at[n], m_recv.at[n], mate) for n in range(2)]
    across = [pass_on(n, rs.at[1], r_recv.at[1], order[n]) for n in range(2)]

    def first_terms(n):
        term = term_of(n)

        @pl.when(inner)
        def _():
            held[n] = term

        @pl.when(jnp.logical_not(inner))
        def _():
            part[n] = term.astype(jnp.bfloat16)
            to_inner[n].start()

    def merge(n):
        @pl.when(inner)
        def _():
            arrived(ms.at[n], r_send.at[n], m_recv.at[n])
            part[n] = (held[n] + ms[n].astype(jnp.float32)).astype(jnp.bfloat16)
            across[n].start()

    first_terms(0)
    first_terms(1)

    @pl.when(inner)
    def _():
        landed(far_outer)
        relays[3].start()

    merge(0)
    part[2] = term_of(2).astype(jnp.bfloat16)
    send(part.at[2], rs.at[0], r_send.at[2], r_recv.at[0], dev(i, mate, c))
    merge(1)
    mine = term_of(3)

    @pl.when(jnp.logical_not(inner))
    def _():
        for h in order[:3]:
            landed(h)

    pieces[diag] = pieces_of(i, code_d, far_scale)
    far = gin.at[:, cols_of(dd, c)]
    send(piece(diag, oc), far, p_send.at[2 * dd + c], p_recv.at[2 * dd + c], dev(i, z, oc))
    keep_far = pltpu.make_async_copy(piece(diag, c), far, load_sem.at[0])
    keep_far.start()

    for n in range(2):
        arrived(rs.at[n], r_send.at[n], r_recv.at[n])
        mine = mine + rs[n].astype(jnp.float32)
    gw[...] = mine * (1.0 / math.sqrt(tok * ni * nj))

    keep.wait()
    keep_far.wait()
    for d in (0,) + near:
        for k, cc in enumerate(cores):
            if d or k:
                ii = peers[d]
                block = gin.at[:, cols_of(ii, cc)]
                arrived(block, p_send.at[2 * ii + cc], p_recv.at[2 * ii + cc])
    arrived(gin.at[:, cols_of(dd, oc)], p_send.at[2 * dd + oc], p_recv.at[2 * dd + oc])
    for cp in sends + across:
        cp.wait_send()

    @pl.when(inner)
    def _():
        for cp in relays:
            cp.wait_send()


def leave(gin, gw, gin_out, gw_out, sem):
    copies = [
        pltpu.make_async_copy(gin, gin_out, sem.at[0]),
        pltpu.make_async_copy(gw, gw_out, sem.at[1]),
    ]
    for cp in copies:
        cp.start()
    for cp in copies:
        cp.wait()


def fused(ni, nj, acts, grad_out, codes, scales):
    tok, width = acts.shape
    kv = grad_out.shape[1]
    rows = codes.shape[0]
    half, nz, blk = rows // 2, nj // 2, rows // nj
    group = 2 * ni
    dma = pltpu.SemaphoreType.DMA
    bf16 = jnp.bfloat16
    anyspace = pl.BlockSpec(memory_space=pl.ANY)
    gin, gw = pl.pallas_call(
        functools.partial(kernel, ni, nj),
        out_shape=(
            pltpu.VMEM((tok, width), bf16),
            pltpu.VMEM((blk, kv), jnp.float32),
        ),
        in_specs=[anyspace] * 4,
        out_specs=(pl.BlockSpec(memory_space=pltpu.VMEM),) * 2,
        scratch_shapes=[
            pltpu.VMEM((group * tok, kv), bf16),
            pltpu.VMEM((tok, width), bf16),
            pltpu.VMEM((half, kv), jnp.int32),
            pltpu.VMEM((1, half // 2), jnp.float32),
            pltpu.VMEM((half, kv), bf16),
            pltpu.VMEM((half, kv), bf16),
            pltpu.VMEM((1, half // 2), jnp.float32),
            pltpu.VMEM((nz, group * tok, blk), bf16),
            pltpu.VMEM((ni, 2 * tok, half), bf16),
            pltpu.VMEM((3, blk, kv), bf16),
            pltpu.VMEM((2, blk, kv), bf16),
            pltpu.VMEM((2, blk, kv), jnp.float32),
            pltpu.VMEM((2, blk, kv), bf16),
            dma((4,)),
            dma((ni,)), dma((group,)), dma((2,)), dma((2,)), dma((ni,)),
            dma((group, nz)), dma((group, nz)),
            dma((group,)), dma((group,)),
            dma((3,)), dma((2,)), dma((2,)),
            dma((6,)), dma((nz,)), dma, dma,
            pltpu.SemaphoreType.REGULAR, pltpu.SemaphoreType.REGULAR,
        ],
        compiler_params=pltpu.CompilerParams(collective_id=0, has_side_effects=True),
    )(acts, grad_out, codes, scales.reshape(1, -1))
    return tuple(pl.pallas_call(
        leave,
        out_shape=(
            jax.ShapeDtypeStruct((tok, width), bf16),
            jax.ShapeDtypeStruct((blk, kv), jnp.float32),
        ),
        in_specs=[anyspace] * 2,
        out_specs=(anyspace,) * 2,
        scratch_shapes=[dma((2,))],
    )(*(pltpu.with_memory_space_constraint(x, pltpu.VMEM) for x in (gin, gw))))


def plain(acts, grad_out, codes, scales):
    rows = codes.shape[0]
    width_kv = codes.shape[1]
    blocks = codes.astype(jnp.float32).reshape(rows // 2, 2 * width_kv) * scales[:, None]
    local_weight = blocks.reshape(rows, width_kv).astype(jnp.bfloat16)
    n_group = lax.axis_size("intra")
    n_cross = lax.axis_size("inter")
    factor = 1.0 / math.sqrt(acts.shape[0] * n_group * n_cross)
    contract = (((0,), (0,)), ((), ()))
    group_cot = lax.all_gather(grad_out, "intra", axis=0, tiled=True)
    columns_owned = lax.all_to_all(acts, "intra", split_axis=1, concat_axis=0, tiled=True)
    grad_w = lax.psum_scatter(
        lax.dot_general(columns_owned, group_cot, contract, preferred_element_type=jnp.float32)
        * factor,
        "inter",
        scatter_dimension=0,
        tiled=True,
    )
    pieces = jnp.dot(group_cot, local_weight.T, preferred_element_type=jnp.float32).astype(
        jnp.bfloat16
    )
    grad_in = lax.all_to_all(pieces, "intra", split_axis=0, concat_axis=1, tiled=True)
    return (grad_in, grad_w)


def solution(mesh):
    ni, nj = mesh.shape["intra"], mesh.shape["inter"]

    def per_device(acts, grad_out, codes, scales):
        rows = codes.shape[0]
        aligned = rows % (nj * 128) == 0 and rows % 512 == 0 and acts.shape[0] % 16 == 0
        if aligned and nj == 8 and ni == 4 and acts.shape[1] == ni * rows:
            return fused(ni, nj, acts, grad_out, codes, scales)
        return plain(acts, grad_out, codes, scales)

    in_specs = (
        P(("intra", "inter"), None),
        P(("intra", "inter"), None),
        P("intra", None),
        P("intra"),
    )
    out_specs = (P(("intra", "inter"), None), P(("intra", "inter"), None))
    return jax.shard_map(
        per_device, mesh=mesh, in_specs=in_specs, out_specs=out_specs, check_vma=False
    )
```

```python
import functools
import math

import jax
import jax.numpy as jnp
from jax import lax
from jax.experimental import pallas as pl
from jax.experimental.pallas import tpu as pltpu
from jax.sharding import PartitionSpec as P

MESH = pl.DeviceIdType.MESH


def flip(index, mask, extent):
    out = 0
    bit = 1
    while bit < extent:
        digit = lax.rem(index // bit, 2)
        out = out + bit * (1 - digit if mask & bit else digit)
        bit *= 2
    return out


def lane_scale(scale_row, half):
    pick = (
        lax.broadcasted_iota(jnp.int32, (half // 2, half), 1) // 2
        == lax.broadcasted_iota(jnp.int32, (half // 2, half), 0)
    ).astype(jnp.float32).astype(jnp.bfloat16)
    rest = jnp.broadcast_to(scale_row, (16, half // 2))
    total = jnp.zeros((16, half), jnp.float32)
    for _ in range(3):
        top = rest.astype(jnp.bfloat16)
        total = total + jnp.dot(top, pick, preferred_element_type=jnp.float32)
        rest = rest - top.astype(jnp.float32)
    return total[0:1]


def kernel(
    ni, nj, acts, go, codes, scales, gin, gw,
    go_all, acts_v, codes_v, scale_v, code_b, code_d, scale_d, ac, pieces, part, rs, held, ms,
    load_sem, go_send, go_recv, pair_recv, gh_send, gh_recv, fw_send, a_send, a_recv, p_send, p_recv,
    r_send, r_recv, m_recv, w_send, w_recv, s_send, s_recv, plane_sem, line_sem,
):
    tok, width = acts.shape
    rows = codes.shape[0]
    half = rows // 2
    nz = nj // 2
    blk = rows // nj
    i = lax.axis_index("intra")
    j = lax.axis_index("inter")
    z = j // 2
    c = lax.rem(j, 2)
    oc = 1 - c
    me = 2 * i + c
    peers = {d: flip(i, d, ni) for d in range(ni)}
    near, diag = (1, 2), 3
    dd = peers[diag]
    cores = (c, oc)
    pair = z // 2
    inner = lax.rem(z, 2) != pair
    mate = 2 * pair + 1 - lax.rem(z, 2)
    far_outer = 3 * (1 - pair)
    far_inner = 2 - pair
    order = [far_outer, far_inner, mate, z]

    def dev(ii, zz, cc):
        return {"intra": ii, "inter": 2 * zz + cc}

    def rdma(src, dst, s, r, where):
        return pltpu.make_async_remote_copy(
            src_ref=src, dst_ref=dst, send_sem=s, recv_sem=r, device_id=where, device_id_type=MESH
        )

    def arrived(ref, s, r):
        rdma(ref, ref, s, r, dev(i, z, oc)).wait_recv()

    sends = []

    def send(*args):
        cp = rdma(*args)
        cp.start()
        sends.append(cp)

    def go_slot(m):
        return go_all.at[pl.ds(pl.multiple_of(m * tok, tok), tok)]

    def go_half(m, n):
        return go_all.at[pl.ds(pl.multiple_of(m * tok + n * (tok // 2), tok // 2), tok // 2)]

    def ac_slot(h, m):
        return ac.at[h, pl.ds(pl.multiple_of(m * tok, tok), tok)]

    def cols_of(ii, cc):
        return pl.ds(pl.multiple_of(ii * rows + cc * half, half), half)

    def quarter(h):
        return pl.ds(pl.multiple_of(h * blk, blk), blk)

    half_start = pl.multiple_of(c * half, half)
    sc_start = pl.multiple_of(c * (half // 2), half // 2)
    barrier = pltpu.get_barrier_semaphore()
    for d in range(1, ni):
        pl.semaphore_signal(barrier, inc=1, device_id=dev(peers[d], z, 0), device_id_type=MESH)

    @pl.when(c == 1)
    def _():
        pl.semaphore_signal(barrier, inc=1, device_id=dev(i, z, 0), device_id_type=MESH)

    load_go = pltpu.make_async_copy(go, go_slot(me), load_sem.at[0])
    load_go.start()
    load_codes = pltpu.make_async_copy(codes.at[pl.ds(half_start, half)], codes_v, load_sem.at[2])
    load_codes.start()
    load_acts = pltpu.make_async_copy(acts, acts_v, load_sem.at[1])
    load_acts.start()
    load_scale = pltpu.make_async_copy(scales.at[:, pl.ds(sc_start, half // 2)], scale_v, load_sem.at[3])
    load_scale.start()
    for k in range(1, nz):
        pl.semaphore_signal(barrier, inc=1, device_id=dev(i, lax.rem(z + k, nz), 1), device_id_type=MESH)

    load_go.wait()

    @pl.when(c == 0)
    def _():
        pl.semaphore_wait(barrier, 2 * ni - 1)
        pl.semaphore_signal(plane_sem, inc=1, device_id=dev(i, z, 1), device_id_type=MESH)

    @pl.when(c == 1)
    def _():
        pl.semaphore_wait(plane_sem, 1)

    def send_go(late):
        for n, d in enumerate(near):
            part_go = go_half(me, 1 - n if late else n)
            send(part_go, part_go, go_send.at[d, late], go_recv.at[me, late], dev(peers[d], z, c))

    send_go(0)

    load_codes.wait()
    code_b[...] = codes_v[...].astype(jnp.float32).astype(jnp.bfloat16)
    load_scale.wait()
    send(scale_v, scale_d, s_send, s_recv, dev(dd, z, c))
    row_scale = lane_scale(scale_v[...], half)
    send(code_b.at[quarter(z)], code_d.at[quarter(z)], w_send.at[0], w_recv.at[z], dev(dd, z, c))
    send_go(1)
    send(go_slot(me), go_slot(me), fw_send.at[0], pair_recv.at[i], dev(i, z, oc))

    load_acts.wait()
    own = []

    def send_columns(h):
        for d in near + (0, diag):
            for k, cc in enumerate(cores):
                ii = peers[d]
                col = pl.multiple_of(ii * rows + (2 * h + cc) * blk, blk)
                src = acts_v.at[:, pl.ds(col, blk)]
                if d or k:
                    m = 2 * ii + cc
                    send(src, ac_slot(h, me), a_send.at[m, h], a_recv.at[me, h], dev(ii, z, cc))
                else:
                    cp = pltpu.make_async_copy(src, ac_slot(h, me), a_recv.at[me, h])
                    cp.start()
                    own.append(cp)

    def wait_pair(ii):
        arrived(go_slot(2 * ii + oc), fw_send.at[0], pair_recv.at[ii])

    for n, d in enumerate(near):
        m = 2 * peers[d] + c
        arrived(go_half(m, n), go_send.at[d, 0], go_recv.at[m, 0])
        send(go_half(m, n), go_half(m, n), gh_send.at[n], gh_recv.at[n], dev(peers[diag ^ d], z, c))
    for h in order:
        send_columns(h)

    @pl.when(c == 1)
    def _():
        pl.semaphore_wait(barrier, 2 * (nz - 1))
        pl.semaphore_signal(line_sem, inc=1, device_id=dev(i, z, 0), device_id_type=MESH)

    @pl.when(c == 0)
    def _():
        pl.semaphore_wait(line_sem, 1)

    def hop(n, h, to):
        return rdma(code_d.at[quarter(h)], code_d.at[quarter(h)], w_send.at[n], w_recv.at[h], dev(i, to, c))

    def landed(h):
        arrived(code_d.at[quarter(h)], w_send.at[0], w_recv.at[h])

    to_mate = hop(1, z, mate)
    relays = [hop(2, z, far_inner), hop(3, mate, far_inner), hop(4, far_inner, mate), hop(5, far_outer, mate)]
    landed(z)
    to_mate.start()
    sends.append(to_mate)

    @pl.when(inner)
    def _():
        relays[0].start()

    for n, d in enumerate(near):
        m = 2 * peers[d] + c
        arrived(go_half(m, 1 - n), go_send.at[d, 1], go_recv.at[m, 1])
        send(go_slot(m), go_slot(m), fw_send.at[d], pair_recv.at[peers[d]], dev(i, z, oc))

    m = 2 * dd + c
    for n in range(2):
        arrived(go_half(m, n), gh_send.at[n], gh_recv.at[n])
    send(go_slot(m), go_slot(m), fw_send.at[diag], pair_recv.at[dd], dev(i, z, oc))

    def pieces_of(ii, code, scale):
        pair = go_all[pl.ds(pl.multiple_of(2 * ii * tok, 2 * tok), 2 * tok)]
        out = lax.dot_general(
            pair, code[...], (((1,), (1,)), ((), ())), preferred_element_type=jnp.float32
        )
        return (out * scale).astype(jnp.bfloat16)

    def piece(n, cc):
        return pieces.at[n, pl.ds(pl.multiple_of(cc * tok, tok), tok)]

    for d in near:
        ii = peers[d]
        wait_pair(ii)
        pieces[d] = pieces_of(ii, code_b, row_scale)
        for cc in cores:
            m = 2 * ii + cc
            send(piece(d, cc), gin.at[:, cols_of(i, c)], p_send.at[m], p_recv.at[me], dev(ii, z, cc))
    wait_pair(i)
    pieces[0] = pieces_of(i, code_b, row_scale)
    send(piece(0, oc), gin.at[:, cols_of(i, c)], p_send.at[2 * i + oc], p_recv.at[me], dev(i, z, oc))
    keep = pltpu.make_async_copy(piece(0, c), gin.at[:, cols_of(i, c)], p_recv.at[me])
    keep.start()

    arrived(scale_d, s_send, s_recv)
    far_scale = lane_scale(scale_d[...], half)
    wait_pair(dd)

    @pl.when(inner)
    def _():
        landed(mate)
        relays[1].start()
        landed(far_inner)
        relays[2].start()

    def term_of(n):
        h = order[n]
        own[n].wait()
        for d in range(ni):
            for k, cc in enumerate(cores):
                if d or k:
                    m = 2 * peers[d] + cc
                    arrived(ac_slot(h, m), a_send.at[m, h], a_recv.at[m, h])
        return lax.dot_general(
            ac[h], go_all[...], (((0,), (0,)), ((), ())), preferred_element_type=jnp.float32
        )

    def pass_on(n, dst, recv, to):
        return rdma(part.at[n], dst, r_send.at[n], recv, dev(i, to, c))

    to_inner = [pass_on(n, ms.at[n], m_recv.at[n], mate) for n in range(2)]
    across = [pass_on(n, rs.at[1], r_recv.at[1], order[n]) for n in range(2)]

    def first_terms(n):
        term = term_of(n)

        @pl.when(inner)
        def _():
            held[n] = term

        @pl.when(jnp.logical_not(inner))
        def _():
            part[n] = term.astype(jnp.bfloat16)
            to_inner[n].start()

    def merge(n):
        @pl.when(inner)
        def _():
            arrived(ms.at[n], r_send.at[n], m_recv.at[n])
            part[n] = (held[n] + ms[n].astype(jnp.float32)).astype(jnp.bfloat16)
            across[n].start()

    first_terms(0)
    first_terms(1)

    @pl.when(inner)
    def _():
        landed(far_outer)
        relays[3].start()

    merge(0)
    part[2] = term_of(2).astype(jnp.bfloat16)
    send(part.at[2], rs.at[0], r_send.at[2], r_recv.at[0], dev(i, mate, c))
    merge(1)
    mine = term_of(3)

    @pl.when(jnp.logical_not(inner))
    def _():
        for h in order[:3]:
            landed(h)

    pieces[diag] = pieces_of(i, code_d, far_scale)
    far = gin.at[:, cols_of(dd, c)]
    send(piece(diag, oc), far, p_send.at[2 * dd + c], p_recv.at[2 * dd + c], dev(i, z, oc))
    keep_far = pltpu.make_async_copy(piece(diag, c), far, load_sem.at[0])
    keep_far.start()

    for n in range(2):
        arrived(rs.at[n], r_send.at[n], r_recv.at[n])
        mine = mine + rs[n].astype(jnp.float32)
    gw[...] = mine * (1.0 / math.sqrt(tok * ni * nj))

    keep.wait()
    keep_far.wait()
    for d in (0,) + near:
        for k, cc in enumerate(cores):
            if d or k:
                ii = peers[d]
                block = gin.at[:, cols_of(ii, cc)]
                arrived(block, p_send.at[2 * ii + cc], p_recv.at[2 * ii + cc])
    arrived(gin.at[:, cols_of(dd, oc)], p_send.at[2 * dd + oc], p_recv.at[2 * dd + oc])
    for cp in sends + across:
        cp.wait_send()

    @pl.when(inner)
    def _():
        for cp in relays:
            cp.wait_send()


def leave(gin, gw, gin_out, gw_out, sem):
    copies = [
        pltpu.make_async_copy(gin, gin_out, sem.at[0]),
        pltpu.make_async_copy(gw, gw_out, sem.at[1]),
    ]
    for cp in copies:
        cp.start()
    for cp in copies:
        cp.wait()


def fused(ni, nj, acts, grad_out, codes, scales):
    tok, width = acts.shape
    kv = grad_out.shape[1]
    rows = codes.shape[0]
    half, nz, blk = rows // 2, nj // 2, rows // nj
    group = 2 * ni
    dma = pltpu.SemaphoreType.DMA
    bf16 = jnp.bfloat16
    anyspace = pl.BlockSpec(memory_space=pl.ANY)
    gin, gw = pl.pallas_call(
        functools.partial(kernel, ni, nj),
        out_shape=(
            pltpu.VMEM((tok, width), bf16),
            pltpu.VMEM((blk, kv), jnp.float32),
        ),
        in_specs=[anyspace] * 4,
        out_specs=(pl.BlockSpec(memory_space=pltpu.VMEM),) * 2,
        scratch_shapes=[
            pltpu.VMEM((group * tok, kv), bf16),
            pltpu.VMEM((tok, width), bf16),
            pltpu.VMEM((half, kv), jnp.int32),
            pltpu.VMEM((1, half // 2), jnp.float32),
            pltpu.VMEM((half, kv), bf16),
            pltpu.VMEM((half, kv), bf16),
            pltpu.VMEM((1, half // 2), jnp.float32),
            pltpu.VMEM((nz, group * tok, blk), bf16),
            pltpu.VMEM((ni, 2 * tok, half), bf16),
            pltpu.VMEM((3, blk, kv), bf16),
            pltpu.VMEM((2, blk, kv), bf16),
            pltpu.VMEM((2, blk, kv), jnp.float32),
            pltpu.VMEM((2, blk, kv), bf16),
            dma((4,)),
            dma((ni, 2)), dma((group, 2)), dma((ni,)), dma((2,)), dma((2,)), dma((ni,)),
            dma((group, nz)), dma((group, nz)),
            dma((group,)), dma((group,)),
            dma((3,)), dma((2,)), dma((2,)),
            dma((6,)), dma((nz,)), dma, dma,
            pltpu.SemaphoreType.REGULAR, pltpu.SemaphoreType.REGULAR,
        ],
        compiler_params=pltpu.CompilerParams(collective_id=0, has_side_effects=True),
    )(acts, grad_out, codes, scales.reshape(1, -1))
    return tuple(pl.pallas_call(
        leave,
        out_shape=(
            jax.ShapeDtypeStruct((tok, width), bf16),
            jax.ShapeDtypeStruct((blk, kv), jnp.float32),
        ),
        in_specs=[anyspace] * 2,
        out_specs=(anyspace,) * 2,
        scratch_shapes=[dma((2,))],
    )(*(pltpu.with_memory_space_constraint(x, pltpu.VMEM) for x in (gin, gw))))


def plain(acts, grad_out, codes, scales):
    rows = codes.shape[0]
    width_kv = codes.shape[1]
    blocks = codes.astype(jnp.float32).reshape(rows // 2, 2 * width_kv) * scales[:, None]
    local_weight = blocks.reshape(rows, width_kv).astype(jnp.bfloat16)
    n_group = lax.axis_size("intra")
    n_cross = lax.axis_size("inter")
    factor = 1.0 / math.sqrt(acts.shape[0] * n_group * n_cross)
    contract = (((0,), (0,)), ((), ()))
    group_cot = lax.all_gather(grad_out, "intra", axis=0, tiled=True)
    columns_owned = lax.all_to_all(acts, "intra", split_axis=1, concat_axis=0, tiled=True)
    grad_w = lax.psum_scatter(
        lax.dot_general(columns_owned, group_cot, contract, preferred_element_type=jnp.float32)
        * factor,
        "inter",
        scatter_dimension=0,
        tiled=True,
    )
    pieces = jnp.dot(group_cot, local_weight.T, preferred_element_type=jnp.float32).astype(
        jnp.bfloat16
    )
    grad_in = lax.all_to_all(pieces, "intra", split_axis=0, concat_axis=1, tiled=True)
    return (grad_in, grad_w)


def solution(mesh):
    ni, nj = mesh.shape["intra"], mesh.shape["inter"]

    def per_device(acts, grad_out, codes, scales):
        rows = codes.shape[0]
        aligned = rows % (nj * 128) == 0 and rows % 512 == 0 and acts.shape[0] % 16 == 0
        if aligned and nj == 8 and ni == 4 and acts.shape[1] == ni * rows:
            return fused(ni, nj, acts, grad_out, codes, scales)
        return plain(acts, grad_out, codes, scales)

    in_specs = (
        P(("intra", "inter"), None),
        P(("intra", "inter"), None),
        P("intra", None),
        P("intra"),
    )
    out_specs = (P(("intra", "inter"), None), P(("intra", "inter"), None))
    return jax.shard_map(
        per_device, mesh=mesh, in_specs=in_specs, out_specs=out_specs, check_vma=False
    )
```

```python
import functools
import math

import jax
import jax.numpy as jnp
from jax import lax
from jax.experimental import pallas as pl
from jax.experimental.pallas import tpu as pltpu
from jax.sharding import PartitionSpec as P

MESH = pl.DeviceIdType.MESH


def flip(index, mask, extent):
    out = 0
    bit = 1
    while bit < extent:
        digit = lax.rem(index // bit, 2)
        out = out + bit * (1 - digit if mask & bit else digit)
        bit *= 2
    return out


def lane_scale(scale_row, half):
    pick = (
        lax.broadcasted_iota(jnp.int32, (half // 2, half), 1) // 2
        == lax.broadcasted_iota(jnp.int32, (half // 2, half), 0)
    ).astype(jnp.float32).astype(jnp.bfloat16)
    rest = jnp.broadcast_to(scale_row, (16, half // 2))
    total = jnp.zeros((16, half), jnp.float32)
    for _ in range(3):
        top = rest.astype(jnp.bfloat16)
        total = total + jnp.dot(top, pick, preferred_element_type=jnp.float32)
        rest = rest - top.astype(jnp.float32)
    return total[0:1]


def kernel(
    ni, nj, acts, go, codes, scales, gin, gw,
    go_all, acts_v, codes_v, scale_v, code_b, code_d, scale_d, ac, pieces, part, rs, held, ms,
    load_sem, go_send, go_recv, pair_recv, gh_recv, a_send, a_recv, p_send, p_recv,
    r_send, r_recv, m_recv, w_send, w_recv, s_send, s_recv, near_sem, diag_sem, line_sem,
):
    tok, width = acts.shape
    rows = codes.shape[0]
    half = rows // 2
    nz = nj // 2
    blk = rows // nj
    i = lax.axis_index("intra")
    j = lax.axis_index("inter")
    z = j // 2
    c = lax.rem(j, 2)
    oc = 1 - c
    me = 2 * i + c
    peers = {d: flip(i, d, ni) for d in range(ni)}
    near, diag = (1, 2), 3
    dd = peers[diag]
    cores = (c, oc)
    pair = z // 2
    inner = lax.rem(z, 2) != pair
    mate = 2 * pair + 1 - lax.rem(z, 2)
    far_outer = 3 * (1 - pair)
    far_inner = 2 - pair
    order = [far_outer, far_inner, mate, z]

    def dev(ii, zz, cc):
        return {"intra": ii, "inter": 2 * zz + cc}

    def rdma(src, dst, s, r, where):
        return pltpu.make_async_remote_copy(
            src_ref=src, dst_ref=dst, send_sem=s, recv_sem=r, device_id=where, device_id_type=MESH
        )

    def arrived(ref, r):
        rdma(ref, ref, r, r, dev(i, z, oc)).wait_recv()

    def drained(ref, s):
        rdma(ref, ref, s, s, dev(i, z, oc)).wait_send()

    def send(*args):
        rdma(*args).start()

    def go_slot(m):
        return go_all.at[pl.ds(pl.multiple_of(m * tok, tok), tok)]

    def go_half(m, n):
        return go_all.at[pl.ds(pl.multiple_of(m * tok + n * (tok // 2), tok // 2), tok // 2)]

    def ac_slot(h, m):
        return ac.at[h, pl.ds(pl.multiple_of(m * tok, tok), tok)]

    def cols_of(ii, cc):
        return pl.ds(pl.multiple_of(ii * rows + cc * half, half), half)

    def quarter(h):
        return pl.ds(pl.multiple_of(h * blk, blk), blk)

    half_start = pl.multiple_of(c * half, half)
    sc_start = pl.multiple_of(c * (half // 2), half // 2)
    barrier = pltpu.get_barrier_semaphore()
    for d in near:
        pl.semaphore_signal(barrier, inc=1, device_id=dev(peers[d], z, 0), device_id_type=MESH)

    @pl.when(c == 1)
    def _():
        pl.semaphore_signal(barrier, inc=1, device_id=dev(i, z, 0), device_id_type=MESH)

    load_go = pltpu.make_async_copy(go, go_slot(me), load_sem.at[0])
    load_go.start()
    load_codes = pltpu.make_async_copy(codes.at[pl.ds(half_start, half)], codes_v, load_sem.at[2])
    load_codes.start()
    load_acts = pltpu.make_async_copy(acts, acts_v, load_sem.at[1])
    load_acts.start()
    load_scale = pltpu.make_async_copy(scales.at[:, pl.ds(sc_start, half // 2)], scale_v, load_sem.at[3])
    load_scale.start()
    for k in range(1, nz):
        pl.semaphore_signal(barrier, inc=1, device_id=dev(i, lax.rem(z + k, nz), 1), device_id_type=MESH)

    load_go.wait()

    @pl.when(c == 0)
    def _():
        pl.semaphore_wait(barrier, 2 * len(near) + 1)
        pl.semaphore_signal(near_sem, inc=1, device_id=dev(i, z, 1), device_id_type=MESH)

    @pl.when(c == 1)
    def _():
        pl.semaphore_wait(near_sem, 1)

    def send_go(late):
        for n, d in enumerate(near):
            part_go = go_half(me, 1 - n if late else n)
            send(part_go, part_go, go_send, go_recv.at[n, late], dev(peers[d], z, c))

    send_go(0)
    pl.semaphore_signal(diag_sem, inc=1, device_id=dev(peers[near[0]], z, c), device_id_type=MESH)

    load_codes.wait()
    code_b[...] = codes_v[...].astype(jnp.float32).astype(jnp.bfloat16)
    load_scale.wait()
    pl.semaphore_wait(diag_sem, 1)
    send(scale_v, scale_d, s_send, s_recv, dev(dd, z, c))
    row_scale = lane_scale(scale_v[...], half)
    send(code_b.at[quarter(z)], code_d.at[quarter(z)], w_send.at[0], w_recv.at[z], dev(dd, z, c))
    send_go(1)
    send(go_slot(me), go_slot(me), go_send, pair_recv.at[0], dev(i, z, oc))

    load_acts.wait()

    def send_columns(n):
        h = order[n]
        for d in near + (0, diag):
            for k, cc in enumerate(cores):
                ii = peers[d]
                col = pl.multiple_of(ii * rows + (2 * h + cc) * blk, blk)
                if d or k:
                    send(acts_v.at[:, pl.ds(col, blk)], ac_slot(h, me), a_send, a_recv.at[n], dev(ii, z, cc))
                else:
                    ac_slot(h, me)[...] = acts_v[:, pl.ds(col, blk)]

    def wait_pair(d):
        arrived(go_slot(2 * peers[d] + oc), pair_recv.at[d])

    for n, d in enumerate(near):
        m = 2 * peers[d] + c
        arrived(go_half(m, n), go_recv.at[n, 0])
        send(go_half(m, n), go_half(m, n), go_send, gh_recv, dev(peers[diag ^ d], z, c))
    for n in range(nz):
        send_columns(n)

    @pl.when(c == 1)
    def _():
        pl.semaphore_wait(barrier, 2 * (nz - 1))
        pl.semaphore_signal(line_sem, inc=1, device_id=dev(i, z, 0), device_id_type=MESH)

    @pl.when(c == 0)
    def _():
        pl.semaphore_wait(line_sem, 1)

    def hop(n, h, to):
        send(code_d.at[quarter(h)], code_d.at[quarter(h)], w_send.at[n], w_recv.at[h], dev(i, to, c))

    def landed(h):
        arrived(code_d.at[quarter(h)], w_recv.at[h])

    landed(z)
    hop(0, z, mate)

    @pl.when(inner)
    def _():
        hop(1, z, far_inner)

    for n, d in enumerate(near):
        m = 2 * peers[d] + c
        arrived(go_half(m, 1 - n), go_recv.at[n, 1])
        send(go_slot(m), go_slot(m), go_send, pair_recv.at[d], dev(i, z, oc))

    m = 2 * dd + c
    arrived(go_slot(m), gh_recv)
    send(go_slot(m), go_slot(m), go_send, pair_recv.at[diag], dev(i, z, oc))

    def pieces_of(ii, code, scale):
        pair = go_all[pl.ds(pl.multiple_of(2 * ii * tok, 2 * tok), 2 * tok)]
        out = lax.dot_general(
            pair, code[...], (((1,), (1,)), ((), ())), preferred_element_type=jnp.float32
        )
        return (out * scale).astype(jnp.bfloat16)

    def piece(n, cc):
        return pieces.at[n, pl.ds(pl.multiple_of(cc * tok, tok), tok)]

    def own_piece(n, ii):
        gin[:, cols_of(ii, c)] = piece(n, c)[...]
        send(piece(n, oc), gin.at[:, cols_of(ii, c)], p_send, p_recv, dev(i, z, oc))

    for d in near:
        ii = peers[d]
        wait_pair(d)
        pieces[d] = pieces_of(ii, code_b, row_scale)
        for cc in cores:
            send(piece(d, cc), gin.at[:, cols_of(i, c)], p_send, p_recv, dev(ii, z, cc))
    wait_pair(0)
    pieces[0] = pieces_of(i, code_b, row_scale)
    own_piece(0, i)

    arrived(scale_d, s_recv)
    far_scale = lane_scale(scale_d[...], half)
    wait_pair(diag)

    @pl.when(inner)
    def _():
        landed(mate)
        hop(1, mate, far_inner)
        hop(1, mate, far_outer)
        landed(far_inner)
        hop(1, far_inner, mate)

    def term_of(n):
        h = order[n]
        arrived(ac.at[h, pl.ds(0, (2 * ni - 1) * tok)], a_recv.at[n])
        return lax.dot_general(
            ac[h], go_all[...], (((0,), (0,)), ((), ())), preferred_element_type=jnp.float32
        )

    def pass_on(n, dst, recv, to):
        send(part.at[n], dst, r_send, recv, dev(i, to, c))

    def first_terms(n):
        term = term_of(n)

        @pl.when(inner)
        def _():
            held[n] = term

        @pl.when(jnp.logical_not(inner))
        def _():
            part[n] = term.astype(jnp.bfloat16)
            pass_on(n, ms.at[n], m_recv.at[n], mate)

    def merge(n):
        @pl.when(inner)
        def _():
            arrived(ms.at[n], m_recv.at[n])
            part[n] = (held[n] + ms[n].astype(jnp.float32)).astype(jnp.bfloat16)
            pass_on(n, rs.at[1], r_recv, order[n])

    first_terms(0)
    first_terms(1)

    merge(0)
    part[2] = term_of(2).astype(jnp.bfloat16)
    pass_on(2, rs.at[0], r_recv, mate)
    merge(1)
    mine = term_of(3)

    @pl.when(jnp.logical_not(inner))
    def _():
        landed(mate)
        landed(far_inner)

    landed(far_outer)

    pieces[diag] = pieces_of(i, code_d, far_scale)
    own_piece(diag, dd)

    arrived(rs, r_recv)
    for n in range(2):
        mine = mine + rs[n].astype(jnp.float32)
    gw[...] = mine * (1.0 / math.sqrt(tok * ni * nj))

    drained(go_all.at[pl.ds(0, (2 * ni - 1) * tok)], go_send)
    drained(acts_v.at[:, pl.ds(0, nz * (2 * ni - 1) * blk)], a_send)
    drained(part, r_send)
    drained(code_d.at[pl.ds(0, 2 * blk)], w_send.at[0])
    drained(scale_v, s_send)

    @pl.when(inner)
    def _():
        drained(code_d, w_send.at[1])

    pieces_all = gin.at[:, pl.ds(0, 6 * half)]
    drained(pieces_all, p_send)
    arrived(pieces_all, p_recv)


def leave(gin, gw, gin_out, gw_out, sem):
    copies = [
        pltpu.make_async_copy(gin, gin_out, sem.at[0]),
        pltpu.make_async_copy(gw, gw_out, sem.at[1]),
    ]
    for cp in copies:
        cp.start()
    for cp in copies:
        cp.wait()


def fused(ni, nj, acts, grad_out, codes, scales):
    tok, width = acts.shape
    kv = grad_out.shape[1]
    rows = codes.shape[0]
    half, nz, blk = rows // 2, nj // 2, rows // nj
    group = 2 * ni
    dma = pltpu.SemaphoreType.DMA
    bf16 = jnp.bfloat16
    anyspace = pl.BlockSpec(memory_space=pl.ANY)
    gin, gw = pl.pallas_call(
        functools.partial(kernel, ni, nj),
        out_shape=(
            pltpu.VMEM((tok, width), bf16),
            pltpu.VMEM((blk, kv), jnp.float32),
        ),
        in_specs=[anyspace] * 4,
        out_specs=(pl.BlockSpec(memory_space=pltpu.VMEM),) * 2,
        scratch_shapes=[
            pltpu.VMEM((group * tok, kv), bf16),
            pltpu.VMEM((tok, width), bf16),
            pltpu.VMEM((half, kv), jnp.int32),
            pltpu.VMEM((1, half // 2), jnp.float32),
            pltpu.VMEM((half, kv), bf16),
            pltpu.VMEM((half, kv), bf16),
            pltpu.VMEM((1, half // 2), jnp.float32),
            pltpu.VMEM((nz, group * tok, blk), bf16),
            pltpu.VMEM((ni, 2 * tok, half), bf16),
            pltpu.VMEM((3, blk, kv), bf16),
            pltpu.VMEM((2, blk, kv), bf16),
            pltpu.VMEM((2, blk, kv), jnp.float32),
            pltpu.VMEM((2, blk, kv), bf16),
            dma((4,)),
            dma, dma((2, 2)), dma((ni,)), dma,
            dma, dma((nz,)), dma, dma,
            dma, dma, dma((2,)),
            dma((2,)), dma((nz,)), dma, dma,
            *[pltpu.SemaphoreType.REGULAR] * 3,
        ],
        compiler_params=pltpu.CompilerParams(collective_id=0, has_side_effects=True),
    )(acts, grad_out, codes, scales.reshape(1, -1))
    return tuple(pl.pallas_call(
        leave,
        out_shape=(
            jax.ShapeDtypeStruct((tok, width), bf16),
            jax.ShapeDtypeStruct((blk, kv), jnp.float32),
        ),
        in_specs=[anyspace] * 2,
        out_specs=(anyspace,) * 2,
        scratch_shapes=[dma((2,))],
    )(*(pltpu.with_memory_space_constraint(x, pltpu.VMEM) for x in (gin, gw))))


def plain(acts, grad_out, codes, scales):
    rows = codes.shape[0]
    width_kv = codes.shape[1]
    blocks = codes.astype(jnp.float32).reshape(rows // 2, 2 * width_kv) * scales[:, None]
    local_weight = blocks.reshape(rows, width_kv).astype(jnp.bfloat16)
    n_group = lax.axis_size("intra")
    n_cross = lax.axis_size("inter")
    factor = 1.0 / math.sqrt(acts.shape[0] * n_group * n_cross)
    contract = (((0,), (0,)), ((), ()))
    group_cot = lax.all_gather(grad_out, "intra", axis=0, tiled=True)
    columns_owned = lax.all_to_all(acts, "intra", split_axis=1, concat_axis=0, tiled=True)
    grad_w = lax.psum_scatter(
        lax.dot_general(columns_owned, group_cot, contract, preferred_element_type=jnp.float32)
        * factor,
        "inter",
        scatter_dimension=0,
        tiled=True,
    )
    pieces = jnp.dot(group_cot, local_weight.T, preferred_element_type=jnp.float32).astype(
        jnp.bfloat16
    )
    grad_in = lax.all_to_all(pieces, "intra", split_axis=0, concat_axis=1, tiled=True)
    return (grad_in, grad_w)


def solution(mesh):
    ni, nj = mesh.shape["intra"], mesh.shape["inter"]

    def per_device(acts, grad_out, codes, scales):
        rows = codes.shape[0]
        aligned = rows % (nj * 128) == 0 and rows % 512 == 0 and acts.shape[0] % 16 == 0
        if aligned and nj == 8 and ni == 4 and acts.shape[1] == ni * rows:
            return fused(ni, nj, acts, grad_out, codes, scales)
        return plain(acts, grad_out, codes, scales)

    in_specs = (
        P(("intra", "inter"), None),
        P(("intra", "inter"), None),
        P("intra", None),
        P("intra"),
    )
    out_specs = (P(("intra", "inter"), None), P(("intra", "inter"), None))
    return jax.shard_map(
        per_device, mesh=mesh, in_specs=in_specs, out_specs=out_specs, check_vma=False
    )
```

```python
import functools
import math

import jax
import jax.numpy as jnp
from jax import lax
from jax.experimental import pallas as pl
from jax.experimental.pallas import tpu as pltpu
from jax.sharding import PartitionSpec as P

MESH = pl.DeviceIdType.MESH


def flip(index, mask, extent):
    out = 0
    bit = 1
    while bit < extent:
        digit = lax.rem(index // bit, 2)
        out = out + bit * (1 - digit if mask & bit else digit)
        bit *= 2
    return out


def lane_scale(scale_row, half):
    pick = (
        lax.broadcasted_iota(jnp.int32, (half // 2, half), 1) // 2
        == lax.broadcasted_iota(jnp.int32, (half // 2, half), 0)
    ).astype(jnp.float32).astype(jnp.bfloat16)
    rest = jnp.broadcast_to(scale_row, (16, half // 2))
    total = jnp.zeros((16, half), jnp.float32)
    for _ in range(3):
        top = rest.astype(jnp.bfloat16)
        total = total + jnp.dot(top, pick, preferred_element_type=jnp.float32)
        rest = rest - top.astype(jnp.float32)
    return total[0:1]


def kernel(
    ni, nj, acts, go, codes, scales, gin, gw,
    go_all, acts_v, codes_v, scale_v, code_b, code_d, scale_d, ac, pieces, part, rs, held, ms,
    load_sem, go_send, go_recv, pair_recv, gh_recv, a_send, a_recv, p_send, p_recv,
    r_send, r_recv, m_recv, w_send, w_recv, s_send, s_recv, near_sem, diag_sem, line_sem,
):
    tok, width = acts.shape
    rows = codes.shape[0]
    half = rows // 2
    nz = nj // 2
    blk = rows // nj
    i = lax.axis_index("intra")
    j = lax.axis_index("inter")
    z = j // 2
    c = lax.rem(j, 2)
    oc = 1 - c
    me = 2 * i + c
    peers = {d: flip(i, d, ni) for d in range(ni)}
    near, diag = (1, 2), 3
    dd = peers[diag]
    cores = (c, oc)
    pair = z // 2
    inner = lax.rem(z, 2) != pair
    mate = 2 * pair + 1 - lax.rem(z, 2)
    far_outer = 3 * (1 - pair)
    far_inner = 2 - pair
    swap = jnp.where(inner, mate - far_inner, 0)
    order = [far_outer, far_inner + swap, mate - swap, z]

    def dev(ii, zz, cc):
        return {"intra": ii, "inter": 2 * zz + cc}

    def rdma(src, dst, s, r, where):
        return pltpu.make_async_remote_copy(
            src_ref=src, dst_ref=dst, send_sem=s, recv_sem=r, device_id=where, device_id_type=MESH
        )

    def arrived(ref, r):
        rdma(ref, ref, r, r, dev(i, z, oc)).wait_recv()

    def drained(ref, s):
        rdma(ref, ref, s, s, dev(i, z, oc)).wait_send()

    def send(*args):
        rdma(*args).start()

    def go_slot(m):
        return go_all.at[pl.ds(pl.multiple_of(m * tok, tok), tok)]

    def go_half(m, n):
        return go_all.at[pl.ds(pl.multiple_of(m * tok + n * (tok // 2), tok // 2), tok // 2)]

    def ac_slot(h, m):
        return ac.at[h, pl.ds(pl.multiple_of(m * tok, tok), tok)]

    def cols_of(ii, cc):
        return pl.ds(pl.multiple_of(ii * rows + cc * half, half), half)

    def quarter(h):
        return pl.ds(pl.multiple_of(h * blk, blk), blk)

    half_start = pl.multiple_of(c * half, half)
    sc_start = pl.multiple_of(c * (half // 2), half // 2)
    barrier = pltpu.get_barrier_semaphore()
    for d in near:
        pl.semaphore_signal(barrier, inc=1, device_id=dev(peers[d], z, 0), device_id_type=MESH)

    @pl.when(c == 1)
    def _():
        pl.semaphore_signal(barrier, inc=1, device_id=dev(i, z, 0), device_id_type=MESH)

    load_go = pltpu.make_async_copy(go, go_slot(me), load_sem.at[0])
    load_go.start()
    load_codes = pltpu.make_async_copy(codes.at[pl.ds(half_start, half)], codes_v, load_sem.at[2])
    load_codes.start()
    load_acts = pltpu.make_async_copy(acts, acts_v, load_sem.at[1])
    load_acts.start()
    load_scale = pltpu.make_async_copy(scales.at[:, pl.ds(sc_start, half // 2)], scale_v, load_sem.at[3])
    load_scale.start()
    for k in range(1, nz):
        pl.semaphore_signal(barrier, inc=1, device_id=dev(i, lax.rem(z + k, nz), 1), device_id_type=MESH)

    load_go.wait()

    @pl.when(c == 0)
    def _():
        pl.semaphore_wait(barrier, 2 * len(near) + 1)
        pl.semaphore_signal(near_sem, inc=1, device_id=dev(i, z, 1), device_id_type=MESH)

    @pl.when(c == 1)
    def _():
        pl.semaphore_wait(near_sem, 1)

    def send_go(late):
        for n, d in enumerate(near):
            part_go = go_half(me, 1 - n if late else n)
            send(part_go, part_go, go_send, go_recv.at[n, late], dev(peers[d], z, c))

    pl.semaphore_signal(diag_sem, inc=1, device_id=dev(peers[near[0]], z, c), device_id_type=MESH)
    send_go(0)
    send_go(1)
    send(go_slot(me), go_slot(me), go_send, pair_recv.at[0], dev(i, z, oc))

    load_codes.wait()
    code_b[...] = codes_v[...].astype(jnp.float32).astype(jnp.bfloat16)
    load_scale.wait()
    pl.semaphore_wait(diag_sem, 1)
    send(scale_v, scale_d, s_send, s_recv, dev(dd, z, c))
    row_scale = lane_scale(scale_v[...], half)
    send(code_b.at[quarter(z)], code_d.at[quarter(z)], w_send.at[0], w_recv.at[z], dev(dd, z, c))

    load_acts.wait()

    def send_columns(n):
        h = order[n]
        for d in near + (0, diag):
            for k, cc in enumerate(cores):
                ii = peers[d]
                col = pl.multiple_of(ii * rows + (2 * h + cc) * blk, blk)
                if d or k:
                    send(acts_v.at[:, pl.ds(col, blk)], ac_slot(h, me), a_send, a_recv.at[n], dev(ii, z, cc))
                else:
                    ac_slot(h, me)[...] = acts_v[:, pl.ds(col, blk)]

    def wait_pair(d):
        arrived(go_slot(2 * peers[d] + oc), pair_recv.at[d])

    for n, d in enumerate(near):
        m = 2 * peers[d] + c
        arrived(go_half(m, n), go_recv.at[n, 0])
        send(go_half(m, n), go_half(m, n), go_send, gh_recv, dev(peers[diag ^ d], z, c))
    for n in range(nz):
        send_columns(n)

    @pl.when(c == 1)
    def _():
        pl.semaphore_wait(barrier, 2 * (nz - 1))
        pl.semaphore_signal(line_sem, inc=1, device_id=dev(i, z, 0), device_id_type=MESH)

    @pl.when(c == 0)
    def _():
        pl.semaphore_wait(line_sem, 1)

    def hop(n, h, to):
        send(code_d.at[quarter(h)], code_d.at[quarter(h)], w_send.at[n], w_recv.at[h], dev(i, to, c))

    def landed(h):
        arrived(code_d.at[quarter(h)], w_recv.at[h])

    landed(z)
    hop(0, z, mate)

    @pl.when(inner)
    def _():
        hop(1, z, far_inner)

    for n, d in enumerate(near):
        m = 2 * peers[d] + c
        arrived(go_half(m, 1 - n), go_recv.at[n, 1])
        send(go_slot(m), go_slot(m), go_send, pair_recv.at[d], dev(i, z, oc))

    m = 2 * dd + c
    arrived(go_slot(m), gh_recv)
    send(go_slot(m), go_slot(m), go_send, pair_recv.at[diag], dev(i, z, oc))

    def pieces_of(ii, code, scale):
        pair = go_all[pl.ds(pl.multiple_of(2 * ii * tok, 2 * tok), 2 * tok)]
        out = lax.dot_general(
            pair, code[...], (((1,), (1,)), ((), ())), preferred_element_type=jnp.float32
        )
        return (out * scale).astype(jnp.bfloat16)

    def piece(n, cc):
        return pieces.at[n, pl.ds(pl.multiple_of(cc * tok, tok), tok)]

    def own_piece(n, ii):
        gin[:, cols_of(ii, c)] = piece(n, c)[...]
        send(piece(n, oc), gin.at[:, cols_of(ii, c)], p_send, p_recv, dev(i, z, oc))

    for d in near:
        ii = peers[d]
        wait_pair(d)
        pieces[d] = pieces_of(ii, code_b, row_scale)
        for cc in cores:
            send(piece(d, cc), gin.at[:, cols_of(i, c)], p_send, p_recv, dev(ii, z, cc))
    wait_pair(0)
    pieces[0] = pieces_of(i, code_b, row_scale)
    own_piece(0, i)

    arrived(scale_d, s_recv)
    far_scale = lane_scale(scale_d[...], half)
    wait_pair(diag)

    @pl.when(inner)
    def _():
        landed(mate)
        hop(1, mate, far_outer)
        landed(far_inner)
        hop(1, far_inner, mate)

    def term_of(n):
        h = order[n]
        arrived(ac.at[h, pl.ds(0, (2 * ni - 1) * tok)], a_recv.at[n])
        return lax.dot_general(
            ac[h], go_all[...], (((0,), (0,)), ((), ())), preferred_element_type=jnp.float32
        )

    def rows_of(q):
        return pl.ds(q * (blk // 2), blk // 2)

    def pass_on(n, q, dst, recv, to):
        send(part.at[n, rows_of(q)], dst.at[rows_of(q)], r_send, recv, dev(i, to, c))

    def give(n, term, dst, recv):
        part[n] = term.astype(jnp.bfloat16)
        for q in range(2):
            pass_on(n, q, dst, recv(q), mate)

    def split(n, on_inner, on_outer):
        term = term_of(n)
        pl.when(inner)(lambda: on_inner(term))
        pl.when(jnp.logical_not(inner))(lambda: on_outer(term))

    def hold(n):
        def keep(term):
            held[n] = term
        return keep

    def to_merge(n):
        return lambda term: give(n, term, ms.at[n], lambda q: m_recv.at[n, q])

    def to_mate(term):
        give(2, term, rs.at[0], lambda q: r_recv)

    def merge(n, to):
        for q in range(2):
            arrived(ms.at[n, rows_of(q)], m_recv.at[n, q])
            total = held[n, rows_of(q)] + ms[n, rows_of(q)].astype(jnp.float32)
            part[n, rows_of(q)] = total.astype(jnp.bfloat16)
            pass_on(n, q, rs.at[1], r_recv, to)

    split(0, hold(0), to_merge(0))
    split(1, to_mate, to_merge(1))

    @pl.when(inner)
    def _():
        merge(0, far_outer)
        hop(1, mate, far_inner)

    split(2, hold(1), to_mate)

    @pl.when(inner)
    def _():
        merge(1, far_inner)

    mine = term_of(3)

    @pl.when(jnp.logical_not(inner))
    def _():
        landed(mate)
        landed(far_inner)

    landed(far_outer)

    pieces[diag] = pieces_of(i, code_d, far_scale)
    own_piece(diag, dd)

    arrived(rs, r_recv)
    for n in range(2):
        mine = mine + rs[n].astype(jnp.float32)
    gw[...] = mine * (1.0 / math.sqrt(tok * ni * nj))

    drained(go_all.at[pl.ds(0, (2 * ni - 1) * tok)], go_send)
    drained(acts_v.at[:, pl.ds(0, nz * (2 * ni - 1) * blk)], a_send)
    drained(part, r_send)
    drained(code_d.at[pl.ds(0, 2 * blk)], w_send.at[0])
    drained(scale_v, s_send)

    @pl.when(inner)
    def _():
        drained(code_d, w_send.at[1])

    pieces_all = gin.at[:, pl.ds(0, 6 * half)]
    drained(pieces_all, p_send)
    arrived(pieces_all, p_recv)


def leave(gin, gw, gin_out, gw_out, sem):
    copies = [
        pltpu.make_async_copy(gin, gin_out, sem.at[0]),
        pltpu.make_async_copy(gw, gw_out, sem.at[1]),
    ]
    for cp in copies:
        cp.start()
    for cp in copies:
        cp.wait()


def fused(ni, nj, acts, grad_out, codes, scales):
    tok, width = acts.shape
    kv = grad_out.shape[1]
    rows = codes.shape[0]
    half, nz, blk = rows // 2, nj // 2, rows // nj
    group = 2 * ni
    dma = pltpu.SemaphoreType.DMA
    bf16 = jnp.bfloat16
    anyspace = pl.BlockSpec(memory_space=pl.ANY)
    gin, gw = pl.pallas_call(
        functools.partial(kernel, ni, nj),
        out_shape=(
            pltpu.VMEM((tok, width), bf16),
            pltpu.VMEM((blk, kv), jnp.float32),
        ),
        in_specs=[anyspace] * 4,
        out_specs=(pl.BlockSpec(memory_space=pltpu.VMEM),) * 2,
        scratch_shapes=[
            pltpu.VMEM((group * tok, kv), bf16),
            pltpu.VMEM((tok, width), bf16),
            pltpu.VMEM((half, kv), jnp.int32),
            pltpu.VMEM((1, half // 2), jnp.float32),
            pltpu.VMEM((half, kv), bf16),
            pltpu.VMEM((half, kv), bf16),
            pltpu.VMEM((1, half // 2), jnp.float32),
            pltpu.VMEM((nz, group * tok, blk), bf16),
            pltpu.VMEM((ni, 2 * tok, half), bf16),
            pltpu.VMEM((3, blk, kv), bf16),
            pltpu.VMEM((2, blk, kv), bf16),
            pltpu.VMEM((2, blk, kv), jnp.float32),
            pltpu.VMEM((2, blk, kv), bf16),
            dma((4,)),
            dma, dma((2, 2)), dma((ni,)), dma,
            dma, dma((nz,)), dma, dma,
            dma, dma, dma((2, 2)),
            dma((2,)), dma((nz,)), dma, dma,
            *[pltpu.SemaphoreType.REGULAR] * 3,
        ],
        compiler_params=pltpu.CompilerParams(collective_id=0, has_side_effects=True),
    )(acts, grad_out, codes, scales.reshape(1, -1))
    return tuple(pl.pallas_call(
        leave,
        out_shape=(
            jax.ShapeDtypeStruct((tok, width), bf16),
            jax.ShapeDtypeStruct((blk, kv), jnp.float32),
        ),
        in_specs=[anyspace] * 2,
        out_specs=(anyspace,) * 2,
        scratch_shapes=[dma((2,))],
    )(*(pltpu.with_memory_space_constraint(x, pltpu.VMEM) for x in (gin, gw))))


def plain(acts, grad_out, codes, scales):
    rows = codes.shape[0]
    width_kv = codes.shape[1]
    blocks = codes.astype(jnp.float32).reshape(rows // 2, 2 * width_kv) * scales[:, None]
    local_weight = blocks.reshape(rows, width_kv).astype(jnp.bfloat16)
    n_group = lax.axis_size("intra")
    n_cross = lax.axis_size("inter")
    factor = 1.0 / math.sqrt(acts.shape[0] * n_group * n_cross)
    contract = (((0,), (0,)), ((), ()))
    group_cot = lax.all_gather(grad_out, "intra", axis=0, tiled=True)
    columns_owned = lax.all_to_all(acts, "intra", split_axis=1, concat_axis=0, tiled=True)
    grad_w = lax.psum_scatter(
        lax.dot_general(columns_owned, group_cot, contract, preferred_element_type=jnp.float32)
        * factor,
        "inter",
        scatter_dimension=0,
        tiled=True,
    )
    pieces = jnp.dot(group_cot, local_weight.T, preferred_element_type=jnp.float32).astype(
        jnp.bfloat16
    )
    grad_in = lax.all_to_all(pieces, "intra", split_axis=0, concat_axis=1, tiled=True)
    return (grad_in, grad_w)


def solution(mesh):
    ni, nj = mesh.shape["intra"], mesh.shape["inter"]

    def per_device(acts, grad_out, codes, scales):
        rows = codes.shape[0]
        aligned = rows % (nj * 128) == 0 and rows % 512 == 0 and acts.shape[0] % 16 == 0
        if aligned and nj == 8 and ni == 4 and acts.shape[1] == ni * rows:
            return fused(ni, nj, acts, grad_out, codes, scales)
        return plain(acts, grad_out, codes, scales)

    in_specs = (
        P(("intra", "inter"), None),
        P(("intra", "inter"), None),
        P("intra", None),
        P("intra"),
    )
    out_specs = (P(("intra", "inter"), None), P(("intra", "inter"), None))
    return jax.shard_map(
        per_device, mesh=mesh, in_specs=in_specs, out_specs=out_specs, check_vma=False
    )
```

```python
import functools
import math

import jax
import jax.numpy as jnp
from jax import lax
from jax.experimental import pallas as pl
from jax.experimental.pallas import tpu as pltpu
from jax.sharding import PartitionSpec as P

MESH = pl.DeviceIdType.MESH


def flip(index, mask, extent):
    out = 0
    bit = 1
    while bit < extent:
        digit = lax.rem(index // bit, 2)
        out = out + bit * (1 - digit if mask & bit else digit)
        bit *= 2
    return out


def lane_scale(scale_row, half):
    pick = (
        lax.broadcasted_iota(jnp.int32, (half // 2, half), 1) // 2
        == lax.broadcasted_iota(jnp.int32, (half // 2, half), 0)
    ).astype(jnp.float32).astype(jnp.bfloat16)
    rest = jnp.broadcast_to(scale_row, (16, half // 2))
    total = jnp.zeros((16, half), jnp.float32)
    for _ in range(3):
        top = rest.astype(jnp.bfloat16)
        total = total + jnp.dot(top, pick, preferred_element_type=jnp.float32)
        rest = rest - top.astype(jnp.float32)
    return total[0:1]


def kernel(
    ni, nj, acts, go, codes, scales, gin, gw,
    go_all, acts_v, codes_v, scale_v, code_b, code_d, scale_d, ac, pieces, part, rs, held, ms,
    load_sem, go_send, go_recv, pair_recv, gh_recv, a_send, a_recv, p_send, p_recv,
    r_send, r_recv, m_recv, w_send, w_recv, s_send, s_recv, near_sem, diag_sem, line_sem,
):
    tok, width = acts.shape
    rows = codes.shape[0]
    half = rows // 2
    nz = nj // 2
    blk = rows // nj
    i = lax.axis_index("intra")
    j = lax.axis_index("inter")
    z = j // 2
    c = lax.rem(j, 2)
    oc = 1 - c
    me = 2 * i + c
    peers = {d: flip(i, d, ni) for d in range(ni)}
    near, diag = (1, 2), 3
    dd = peers[diag]
    cores = (c, oc)
    pair = z // 2
    inner = lax.rem(z, 2) != pair
    mate = 2 * pair + 1 - lax.rem(z, 2)
    far_outer = 3 * (1 - pair)
    far_inner = 2 - pair
    swap = jnp.where(inner, mate - far_inner, 0)
    order = [far_outer, far_inner + swap, mate - swap, z]

    def dev(ii, zz, cc):
        return {"intra": ii, "inter": 2 * zz + cc}

    def rdma(src, dst, s, r, where):
        return pltpu.make_async_remote_copy(
            src_ref=src, dst_ref=dst, send_sem=s, recv_sem=r, device_id=where, device_id_type=MESH
        )

    def arrived(ref, r):
        rdma(ref, ref, r, r, dev(i, z, oc)).wait_recv()

    def drained(ref, s):
        rdma(ref, ref, s, s, dev(i, z, oc)).wait_send()

    def send(*args):
        rdma(*args).start()

    def go_slot(m):
        return go_all.at[pl.ds(pl.multiple_of(m * tok, tok), tok)]

    def go_half(m, n):
        return go_all.at[pl.ds(pl.multiple_of(m * tok + n * (tok // 2), tok // 2), tok // 2)]

    def ac_slot(h, m):
        return ac.at[h, pl.ds(pl.multiple_of(m * tok, tok), tok)]

    def cols_of(ii, cc):
        return pl.ds(pl.multiple_of(ii * rows + cc * half, half), half)

    def quarter(h, q):
        return pl.ds(pl.multiple_of(h * blk + q * (blk // 2), blk // 2), blk // 2)

    half_start = pl.multiple_of(c * half, half)
    sc_start = pl.multiple_of(c * (half // 2), half // 2)
    barrier = pltpu.get_barrier_semaphore()
    for d in near:
        pl.semaphore_signal(barrier, inc=1, device_id=dev(peers[d], z, 0), device_id_type=MESH)

    @pl.when(c == 1)
    def _():
        pl.semaphore_signal(barrier, inc=1, device_id=dev(i, z, 0), device_id_type=MESH)

    load_go = pltpu.make_async_copy(go, go_slot(me), load_sem.at[0])
    load_go.start()
    load_codes = pltpu.make_async_copy(codes.at[pl.ds(half_start, half)], codes_v, load_sem.at[2])
    load_codes.start()
    load_acts = pltpu.make_async_copy(acts, acts_v, load_sem.at[1])
    load_acts.start()
    load_scale = pltpu.make_async_copy(scales.at[:, pl.ds(sc_start, half // 2)], scale_v, load_sem.at[3])
    load_scale.start()
    for k in range(1, nz):
        pl.semaphore_signal(barrier, inc=1, device_id=dev(i, lax.rem(z + k, nz), 1), device_id_type=MESH)

    load_go.wait()

    @pl.when(c == 0)
    def _():
        pl.semaphore_wait(barrier, 2 * len(near) + 1)
        pl.semaphore_signal(near_sem, inc=1, device_id=dev(i, z, 1), device_id_type=MESH)

    @pl.when(c == 1)
    def _():
        pl.semaphore_wait(near_sem, 1)

    def send_go(late):
        for n, d in enumerate(near):
            part_go = go_half(me, 1 - n if late else n)
            send(part_go, part_go, go_send, go_recv.at[n, late], dev(peers[d], z, c))

    pl.semaphore_signal(diag_sem, inc=1, device_id=dev(peers[near[0]], z, c), device_id_type=MESH)
    send_go(0)
    send_go(1)
    send(go_slot(me), go_slot(me), go_send, pair_recv.at[0], dev(i, z, oc))

    load_codes.wait()
    code_b[...] = codes_v[...].astype(jnp.float32).astype(jnp.bfloat16)
    load_scale.wait()
    pl.semaphore_wait(diag_sem, 1)
    send(scale_v, scale_d, s_send, s_recv, dev(dd, z, c))
    row_scale = lane_scale(scale_v[...], half)
    for q in range(2):
        send(code_b.at[quarter(z, q)], code_d.at[quarter(z, q)], w_send.at[0], w_recv.at[z, q], dev(dd, z, c))

    load_acts.wait()

    def send_columns(n):
        h = order[n]
        for d in near + (0, diag):
            for k, cc in enumerate(cores):
                ii = peers[d]
                col = pl.multiple_of(ii * rows + (2 * h + cc) * blk, blk)
                if d or k:
                    send(acts_v.at[:, pl.ds(col, blk)], ac_slot(h, me), a_send, a_recv.at[n], dev(ii, z, cc))
                else:
                    ac_slot(h, me)[...] = acts_v[:, pl.ds(col, blk)]

    def wait_pair(d):
        arrived(go_slot(2 * peers[d] + oc), pair_recv.at[d])

    for n, d in enumerate(near):
        m = 2 * peers[d] + c
        arrived(go_half(m, n), go_recv.at[n, 0])
        send(go_half(m, n), go_half(m, n), go_send, gh_recv, dev(peers[diag ^ d], z, c))
    for n in range(nz):
        send_columns(n)

    @pl.when(c == 1)
    def _():
        pl.semaphore_wait(barrier, 2 * (nz - 1))
        pl.semaphore_signal(line_sem, inc=1, device_id=dev(i, z, 0), device_id_type=MESH)

    @pl.when(c == 0)
    def _():
        pl.semaphore_wait(line_sem, 1)

    def hop(n, h, q, to):
        send(code_d.at[quarter(h, q)], code_d.at[quarter(h, q)], w_send.at[n], w_recv.at[h, q], dev(i, to, c))

    def landed(h, q):
        arrived(code_d.at[quarter(h, q)], w_recv.at[h, q])

    for q in range(2):
        landed(z, q)
        hop(0, z, q, mate)

        @pl.when(inner)
        def _():
            hop(1, z, q, far_inner)

    for n, d in enumerate(near):
        m = 2 * peers[d] + c
        arrived(go_half(m, 1 - n), go_recv.at[n, 1])
        send(go_slot(m), go_slot(m), go_send, pair_recv.at[d], dev(i, z, oc))

    m = 2 * dd + c
    arrived(go_slot(m), gh_recv)
    send(go_slot(m), go_slot(m), go_send, pair_recv.at[diag], dev(i, z, oc))

    def pieces_of(ii, code, scale):
        pair = go_all[pl.ds(pl.multiple_of(2 * ii * tok, 2 * tok), 2 * tok)]
        out = lax.dot_general(
            pair, code[...], (((1,), (1,)), ((), ())), preferred_element_type=jnp.float32
        )
        return (out * scale).astype(jnp.bfloat16)

    def piece(n, cc):
        return pieces.at[n, pl.ds(pl.multiple_of(cc * tok, tok), tok)]

    def own_piece(n, ii):
        gin[:, cols_of(ii, c)] = piece(n, c)[...]
        send(piece(n, oc), gin.at[:, cols_of(ii, c)], p_send, p_recv, dev(i, z, oc))

    for d in near:
        ii = peers[d]
        wait_pair(d)
        pieces[d] = pieces_of(ii, code_b, row_scale)
        for cc in cores:
            send(piece(d, cc), gin.at[:, cols_of(i, c)], p_send, p_recv, dev(ii, z, cc))
    wait_pair(0)
    pieces[0] = pieces_of(i, code_b, row_scale)
    own_piece(0, i)

    arrived(scale_d, s_recv)
    far_scale = lane_scale(scale_d[...], half)
    wait_pair(diag)

    @pl.when(inner)
    def _():
        for q in range(2):
            landed(mate, q)
            hop(1, mate, q, far_outer)
        for q in range(2):
            hop(1, mate, q, far_inner)
        for q in range(2):
            landed(far_inner, q)
            hop(1, far_inner, q, mate)

    def term_of(n):
        h = order[n]
        arrived(ac.at[h, pl.ds(0, (2 * ni - 1) * tok)], a_recv.at[n])
        return lax.dot_general(
            ac[h], go_all[...], (((0,), (0,)), ((), ())), preferred_element_type=jnp.float32
        )

    def rows_of(q):
        return pl.ds(q * (blk // 2), blk // 2)

    def pass_on(n, q, dst, recv, to):
        send(part.at[n, rows_of(q)], dst.at[rows_of(q)], r_send, recv, dev(i, to, c))

    def give(n, term, dst, recv):
        part[n] = term.astype(jnp.bfloat16)
        for q in range(2):
            pass_on(n, q, dst, recv(q), mate)

    def split(n, on_inner, on_outer):
        term = term_of(n)
        pl.when(inner)(lambda: on_inner(term))
        pl.when(jnp.logical_not(inner))(lambda: on_outer(term))

    def hold(n):
        def keep(term):
            held[n] = term
        return keep

    def to_merge(n):
        return lambda term: give(n, term, ms.at[n], lambda q: m_recv.at[n, q])

    def to_mate(term):
        give(2, term, rs.at[0], lambda q: r_recv)

    def merge(n, to):
        for q in range(2):
            arrived(ms.at[n, rows_of(q)], m_recv.at[n, q])
            total = held[n, rows_of(q)] + ms[n, rows_of(q)].astype(jnp.float32)
            part[n, rows_of(q)] = total.astype(jnp.bfloat16)
            pass_on(n, q, rs.at[1], r_recv, to)

    split(0, hold(0), to_merge(0))
    split(1, to_mate, to_merge(1))

    @pl.when(inner)
    def _():
        merge(0, far_outer)

    split(2, hold(1), to_mate)

    @pl.when(inner)
    def _():
        merge(1, far_inner)

    mine = term_of(3)

    @pl.when(jnp.logical_not(inner))
    def _():
        for q in range(2):
            landed(mate, q)
            landed(far_inner, q)

    for q in range(2):
        landed(far_outer, q)

    pieces[diag] = pieces_of(i, code_d, far_scale)
    own_piece(diag, dd)

    arrived(rs, r_recv)
    for n in range(2):
        mine = mine + rs[n].astype(jnp.float32)
    gw[...] = mine * (1.0 / math.sqrt(tok * ni * nj))

    drained(go_all.at[pl.ds(0, (2 * ni - 1) * tok)], go_send)
    drained(acts_v.at[:, pl.ds(0, nz * (2 * ni - 1) * blk)], a_send)
    drained(part, r_send)
    drained(code_d.at[pl.ds(0, 2 * blk)], w_send.at[0])
    drained(scale_v, s_send)

    @pl.when(inner)
    def _():
        drained(code_d, w_send.at[1])

    pieces_all = gin.at[:, pl.ds(0, 6 * half)]
    drained(pieces_all, p_send)
    arrived(pieces_all, p_recv)


def leave(gin, gw, gin_out, gw_out, sem):
    copies = [
        pltpu.make_async_copy(gin, gin_out, sem.at[0]),
        pltpu.make_async_copy(gw, gw_out, sem.at[1]),
    ]
    for cp in copies:
        cp.start()
    for cp in copies:
        cp.wait()


def fused(ni, nj, acts, grad_out, codes, scales):
    tok, width = acts.shape
    kv = grad_out.shape[1]
    rows = codes.shape[0]
    half, nz, blk = rows // 2, nj // 2, rows // nj
    group = 2 * ni
    dma = pltpu.SemaphoreType.DMA
    bf16 = jnp.bfloat16
    anyspace = pl.BlockSpec(memory_space=pl.ANY)
    gin, gw = pl.pallas_call(
        functools.partial(kernel, ni, nj),
        out_shape=(
            pltpu.VMEM((tok, width), bf16),
            pltpu.VMEM((blk, kv), jnp.float32),
        ),
        in_specs=[anyspace] * 4,
        out_specs=(pl.BlockSpec(memory_space=pltpu.VMEM),) * 2,
        scratch_shapes=[
            pltpu.VMEM((group * tok, kv), bf16),
            pltpu.VMEM((tok, width), bf16),
            pltpu.VMEM((half, kv), jnp.int32),
            pltpu.VMEM((1, half // 2), jnp.float32),
            pltpu.VMEM((half, kv), bf16),
            pltpu.VMEM((half, kv), bf16),
            pltpu.VMEM((1, half // 2), jnp.float32),
            pltpu.VMEM((nz, group * tok, blk), bf16),
            pltpu.VMEM((ni, 2 * tok, half), bf16),
            pltpu.VMEM((3, blk, kv), bf16),
            pltpu.VMEM((2, blk, kv), bf16),
            pltpu.VMEM((2, blk, kv), jnp.float32),
            pltpu.VMEM((2, blk, kv), bf16),
            dma((4,)),
            dma, dma((2, 2)), dma((ni,)), dma,
            dma, dma((nz,)), dma, dma,
            dma, dma, dma((2, 2)),
            dma((2,)), dma((nz, 2)), dma, dma,
            *[pltpu.SemaphoreType.REGULAR] * 3,
        ],
        compiler_params=pltpu.CompilerParams(collective_id=0, has_side_effects=True),
    )(acts, grad_out, codes, scales.reshape(1, -1))
    return tuple(pl.pallas_call(
        leave,
        out_shape=(
            jax.ShapeDtypeStruct((tok, width), bf16),
            jax.ShapeDtypeStruct((blk, kv), jnp.float32),
        ),
        in_specs=[anyspace] * 2,
        out_specs=(anyspace,) * 2,
        scratch_shapes=[dma((2,))],
    )(*(pltpu.with_memory_space_constraint(x, pltpu.VMEM) for x in (gin, gw))))


def plain(acts, grad_out, codes, scales):
    rows = codes.shape[0]
    width_kv = codes.shape[1]
    blocks = codes.astype(jnp.float32).reshape(rows // 2, 2 * width_kv) * scales[:, None]
    local_weight = blocks.reshape(rows, width_kv).astype(jnp.bfloat16)
    n_group = lax.axis_size("intra")
    n_cross = lax.axis_size("inter")
    factor = 1.0 / math.sqrt(acts.shape[0] * n_group * n_cross)
    contract = (((0,), (0,)), ((), ()))
    group_cot = lax.all_gather(grad_out, "intra", axis=0, tiled=True)
    columns_owned = lax.all_to_all(acts, "intra", split_axis=1, concat_axis=0, tiled=True)
    grad_w = lax.psum_scatter(
        lax.dot_general(columns_owned, group_cot, contract, preferred_element_type=jnp.float32)
        * factor,
        "inter",
        scatter_dimension=0,
        tiled=True,
    )
    pieces = jnp.dot(group_cot, local_weight.T, preferred_element_type=jnp.float32).astype(
        jnp.bfloat16
    )
    grad_in = lax.all_to_all(pieces, "intra", split_axis=0, concat_axis=1, tiled=True)
    return (grad_in, grad_w)


def solution(mesh):
    ni, nj = mesh.shape["intra"], mesh.shape["inter"]

    def per_device(acts, grad_out, codes, scales):
        rows = codes.shape[0]
        aligned = rows % (nj * 128) == 0 and rows % 512 == 0 and acts.shape[0] % 16 == 0
        if aligned and nj == 8 and ni == 4 and acts.shape[1] == ni * rows:
            return fused(ni, nj, acts, grad_out, codes, scales)
        return plain(acts, grad_out, codes, scales)

    in_specs = (
        P(("intra", "inter"), None),
        P(("intra", "inter"), None),
        P("intra", None),
        P("intra"),
    )
    out_specs = (P(("intra", "inter"), None), P(("intra", "inter"), None))
    return jax.shard_map(
        per_device, mesh=mesh, in_specs=in_specs, out_specs=out_specs, check_vma=False
    )
```

```python
import functools
import math

import jax
import jax.numpy as jnp
from jax import lax
from jax.experimental import pallas as pl
from jax.experimental.pallas import tpu as pltpu
from jax.sharding import PartitionSpec as P

MESH = pl.DeviceIdType.MESH


def flip(index, mask, extent):
    out = 0
    bit = 1
    while bit < extent:
        digit = lax.rem(index // bit, 2)
        out = out + bit * (1 - digit if mask & bit else digit)
        bit *= 2
    return out


def lane_scale(scale_row, half):
    pick = (
        lax.broadcasted_iota(jnp.int32, (half // 2, half), 1) // 2
        == lax.broadcasted_iota(jnp.int32, (half // 2, half), 0)
    ).astype(jnp.float32).astype(jnp.bfloat16)
    rest = jnp.broadcast_to(scale_row, (16, half // 2))
    total = jnp.zeros((16, half), jnp.float32)
    for _ in range(3):
        top = rest.astype(jnp.bfloat16)
        total = total + jnp.dot(top, pick, preferred_element_type=jnp.float32)
        rest = rest - top.astype(jnp.float32)
    return total[0:1]


def kernel(
    ni, nj, acts, go, codes, scales, gin, gw,
    go_all, acts_v, codes_v, scale_v, code_b, code_d, scale_d, ac, pieces, part, rs, held, ms,
    load_sem, go_send, go_recv, pair_recv, gh_recv, a_send, a_recv, p_send, p_recv,
    r_send, r_recv, m_recv, w_send, w_recv, s_send, s_recv, near_sem, diag_sem, line_sem,
):
    tok, width = acts.shape
    rows = codes.shape[0]
    half = rows // 2
    nz = nj // 2
    blk = rows // nj
    i = lax.axis_index("intra")
    j = lax.axis_index("inter")
    z = j // 2
    c = lax.rem(j, 2)
    oc = 1 - c
    me = 2 * i + c
    peers = {d: flip(i, d, ni) for d in range(ni)}
    near, diag = (1, 2), 3
    dd = peers[diag]
    cores = (c, oc)
    pair = z // 2
    inner = lax.rem(z, 2) != pair
    mate = 2 * pair + 1 - lax.rem(z, 2)
    far_outer = 3 * (1 - pair)
    far_inner = 2 - pair
    swap = jnp.where(inner, mate - far_inner, 0)
    order = [far_outer, far_inner + swap, mate - swap, z]

    def dev(ii, zz, cc):
        return {"intra": ii, "inter": 2 * zz + cc}

    def rdma(src, dst, s, r, where):
        return pltpu.make_async_remote_copy(
            src_ref=src, dst_ref=dst, send_sem=s, recv_sem=r, device_id=where, device_id_type=MESH
        )

    def arrived(ref, r):
        rdma(ref, ref, r, r, dev(i, z, oc)).wait_recv()

    def drained(ref, s):
        rdma(ref, ref, s, s, dev(i, z, oc)).wait_send()

    def send(*args):
        rdma(*args).start()

    def go_slot(m):
        return go_all.at[pl.ds(pl.multiple_of(m * tok, tok), tok)]

    def go_half(m, n):
        return go_all.at[pl.ds(pl.multiple_of(m * tok + n * (tok // 2), tok // 2), tok // 2)]

    def ac_slot(h, m):
        return ac.at[h, pl.ds(pl.multiple_of(m * tok, tok), tok)]

    def cols_of(ii, cc):
        return pl.ds(pl.multiple_of(ii * rows + cc * half, half), half)

    less = blk * 3 // 4
    share = {False: less, True: 2 * blk - less}

    def shares(h, q, big):
        start = (h // 2) * (2 * blk) + lax.rem(h, 2) * share[not big] + q * (share[big] // 2)
        return pl.ds(pl.multiple_of(start, 16), share[big] // 2)

    def by_kind(work):
        pl.when(inner)(lambda: work(True))
        pl.when(jnp.logical_not(inner))(lambda: work(False))

    half_start = pl.multiple_of(c * half, half)
    sc_start = pl.multiple_of(c * (half // 2), half // 2)
    barrier = pltpu.get_barrier_semaphore()
    for d in near:
        pl.semaphore_signal(barrier, inc=1, device_id=dev(peers[d], z, 0), device_id_type=MESH)

    @pl.when(c == 1)
    def _():
        pl.semaphore_signal(barrier, inc=1, device_id=dev(i, z, 0), device_id_type=MESH)

    load_go = pltpu.make_async_copy(go, go_slot(me), load_sem.at[0])
    load_go.start()
    load_codes = pltpu.make_async_copy(codes.at[pl.ds(half_start, half)], codes_v, load_sem.at[2])
    load_codes.start()
    load_acts = pltpu.make_async_copy(acts, acts_v, load_sem.at[1])
    load_acts.start()
    load_scale = pltpu.make_async_copy(scales.at[:, pl.ds(sc_start, half // 2)], scale_v, load_sem.at[3])
    load_scale.start()
    for k in range(1, nz):
        pl.semaphore_signal(barrier, inc=1, device_id=dev(i, lax.rem(z + k, nz), 1), device_id_type=MESH)

    load_go.wait()

    @pl.when(c == 0)
    def _():
        pl.semaphore_wait(barrier, 2 * len(near) + 1)
        pl.semaphore_signal(near_sem, inc=1, device_id=dev(i, z, 1), device_id_type=MESH)

    @pl.when(c == 1)
    def _():
        pl.semaphore_wait(near_sem, 1)

    def send_go(late):
        for n, d in enumerate(near):
            part_go = go_half(me, 1 - n if late else n)
            send(part_go, part_go, go_send, go_recv.at[n, late], dev(peers[d], z, c))

    pl.semaphore_signal(diag_sem, inc=1, device_id=dev(peers[near[0]], z, c), device_id_type=MESH)
    send_go(0)
    send_go(1)
    send(go_slot(me), go_slot(me), go_send, pair_recv.at[0], dev(i, z, oc))

    load_codes.wait()
    code_b[...] = codes_v[...].astype(jnp.float32).astype(jnp.bfloat16)
    load_scale.wait()
    pl.semaphore_wait(diag_sem, 1)
    send(scale_v, scale_d, s_send, s_recv, dev(dd, z, c))
    row_scale = lane_scale(scale_v[...], half)

    @by_kind
    def _(big):
        for q in range(2):
            rows_q = shares(z, q, big)
            send(code_b.at[rows_q], code_d.at[rows_q], w_send.at[0], w_recv.at[z, q], dev(dd, z, c))


    load_acts.wait()

    def send_columns(n):
        h = order[n]
        for d in near + (0, diag):
            for k, cc in enumerate(cores):
                ii = peers[d]
                col = pl.multiple_of(ii * rows + (2 * h + cc) * blk, blk)
                if d or k:
                    send(acts_v.at[:, pl.ds(col, blk)], ac_slot(h, me), a_send, a_recv.at[n], dev(ii, z, cc))
                else:
                    ac_slot(h, me)[...] = acts_v[:, pl.ds(col, blk)]

    def wait_pair(d):
        arrived(go_slot(2 * peers[d] + oc), pair_recv.at[d])

    for n, d in enumerate(near):
        m = 2 * peers[d] + c
        arrived(go_half(m, n), go_recv.at[n, 0])
        send(go_half(m, n), go_half(m, n), go_send, gh_recv, dev(peers[diag ^ d], z, c))
    for n in range(nz):
        send_columns(n)

    @pl.when(c == 1)
    def _():
        pl.semaphore_wait(barrier, 2 * (nz - 1))
        pl.semaphore_signal(line_sem, inc=1, device_id=dev(i, z, 0), device_id_type=MESH)

    @pl.when(c == 0)
    def _():
        pl.semaphore_wait(line_sem, 1)

    def hop(n, h, q, big, to):
        rows_q = code_d.at[shares(h, q, big)]
        send(rows_q, rows_q, w_send.at[n], w_recv.at[h, q], dev(i, to, c))

    def landed(h, q, big):
        arrived(code_d.at[shares(h, q, big)], w_recv.at[h, q])

    @by_kind
    def _(big):
        for q in range(2):
            landed(z, q, big)
            hop(0, z, q, big, mate)
            if big:
                hop(1, z, q, big, far_inner)

    for n, d in enumerate(near):
        m = 2 * peers[d] + c
        arrived(go_half(m, 1 - n), go_recv.at[n, 1])
        send(go_slot(m), go_slot(m), go_send, pair_recv.at[d], dev(i, z, oc))

    m = 2 * dd + c
    arrived(go_slot(m), gh_recv)
    send(go_slot(m), go_slot(m), go_send, pair_recv.at[diag], dev(i, z, oc))

    def pieces_of(ii, code, scale):
        pair = go_all[pl.ds(pl.multiple_of(2 * ii * tok, 2 * tok), 2 * tok)]
        out = lax.dot_general(
            pair, code[...], (((1,), (1,)), ((), ())), preferred_element_type=jnp.float32
        )
        return (out * scale).astype(jnp.bfloat16)

    def piece(n, cc):
        return pieces.at[n, pl.ds(pl.multiple_of(cc * tok, tok), tok)]

    def own_piece(n, ii):
        gin[:, cols_of(ii, c)] = piece(n, c)[...]
        send(piece(n, oc), gin.at[:, cols_of(ii, c)], p_send, p_recv, dev(i, z, oc))

    for d in near:
        ii = peers[d]
        wait_pair(d)
        pieces[d] = pieces_of(ii, code_b, row_scale)
        for cc in cores:
            send(piece(d, cc), gin.at[:, cols_of(i, c)], p_send, p_recv, dev(ii, z, cc))
    wait_pair(0)
    pieces[0] = pieces_of(i, code_b, row_scale)
    own_piece(0, i)

    arrived(scale_d, s_recv)
    far_scale = lane_scale(scale_d[...], half)
    wait_pair(diag)

    @pl.when(inner)
    def _():
        for q in range(2):
            landed(mate, q, False)
            hop(1, mate, q, False, far_outer)
        for q in range(2):
            hop(1, mate, q, False, far_inner)
        for q in range(2):
            landed(far_inner, q, True)
            hop(1, far_inner, q, True, mate)

    def term_of(n):
        h = order[n]
        arrived(ac.at[h, pl.ds(0, (2 * ni - 1) * tok)], a_recv.at[n])
        return lax.dot_general(
            ac[h], go_all[...], (((0,), (0,)), ((), ())), preferred_element_type=jnp.float32
        )

    def rows_of(q):
        return pl.ds(q * (blk // 2), blk // 2)

    def pass_on(n, q, dst, recv, to):
        send(part.at[n, rows_of(q)], dst.at[rows_of(q)], r_send, recv, dev(i, to, c))

    def give(n, term, dst, recv):
        part[n] = term.astype(jnp.bfloat16)
        for q in range(2):
            pass_on(n, q, dst, recv(q), mate)

    def split(n, on_inner, on_outer):
        term = term_of(n)
        pl.when(inner)(lambda: on_inner(term))
        pl.when(jnp.logical_not(inner))(lambda: on_outer(term))

    def hold(n):
        def keep(term):
            held[n] = term
        return keep

    def to_merge(n):
        return lambda term: give(n, term, ms.at[n], lambda q: m_recv.at[n, q])

    def to_mate(term):
        give(2, term, rs.at[0], lambda q: r_recv)

    def merge(n, to):
        for q in range(2):
            arrived(ms.at[n, rows_of(q)], m_recv.at[n, q])
            total = held[n, rows_of(q)] + ms[n, rows_of(q)].astype(jnp.float32)
            part[n, rows_of(q)] = total.astype(jnp.bfloat16)
            pass_on(n, q, rs.at[1], r_recv, to)

    split(0, hold(0), to_merge(0))
    split(1, to_mate, to_merge(1))

    @pl.when(inner)
    def _():
        merge(0, far_outer)

    split(2, hold(1), to_mate)

    @pl.when(inner)
    def _():
        merge(1, far_inner)

    mine = term_of(3)

    @pl.when(jnp.logical_not(inner))
    def _():
        for q in range(2):
            landed(mate, q, True)
            landed(far_inner, q, True)

    for q in range(2):
        landed(far_outer, q, False)

    pieces[diag] = pieces_of(i, code_d, far_scale)
    own_piece(diag, dd)

    arrived(rs, r_recv)
    for n in range(2):
        mine = mine + rs[n].astype(jnp.float32)
    gw[...] = mine * (1.0 / math.sqrt(tok * ni * nj))

    drained(go_all.at[pl.ds(0, (2 * ni - 1) * tok)], go_send)
    drained(acts_v.at[:, pl.ds(0, nz * (2 * ni - 1) * blk)], a_send)
    drained(part, r_send)
    drained(scale_v, s_send)

    @by_kind
    def _(big):
        drained(code_d.at[pl.ds(0, 2 * share[big])], w_send.at[0])
        if big:
            drained(code_d, w_send.at[1])

    pieces_all = gin.at[:, pl.ds(0, 6 * half)]
    drained(pieces_all, p_send)
    arrived(pieces_all, p_recv)


def leave(gin, gw, gin_out, gw_out, sem):
    copies = [
        pltpu.make_async_copy(gin, gin_out, sem.at[0]),
        pltpu.make_async_copy(gw, gw_out, sem.at[1]),
    ]
    for cp in copies:
        cp.start()
    for cp in copies:
        cp.wait()


def fused(ni, nj, acts, grad_out, codes, scales):
    tok, width = acts.shape
    kv = grad_out.shape[1]
    rows = codes.shape[0]
    half, nz, blk = rows // 2, nj // 2, rows // nj
    group = 2 * ni
    dma = pltpu.SemaphoreType.DMA
    bf16 = jnp.bfloat16
    anyspace = pl.BlockSpec(memory_space=pl.ANY)
    gin, gw = pl.pallas_call(
        functools.partial(kernel, ni, nj),
        out_shape=(
            pltpu.VMEM((tok, width), bf16),
            pltpu.VMEM((blk, kv), jnp.float32),
        ),
        in_specs=[anyspace] * 4,
        out_specs=(pl.BlockSpec(memory_space=pltpu.VMEM),) * 2,
        scratch_shapes=[
            pltpu.VMEM((group * tok, kv), bf16),
            pltpu.VMEM((tok, width), bf16),
            pltpu.VMEM((half, kv), jnp.int32),
            pltpu.VMEM((1, half // 2), jnp.float32),
            pltpu.VMEM((half, kv), bf16),
            pltpu.VMEM((half, kv), bf16),
            pltpu.VMEM((1, half // 2), jnp.float32),
            pltpu.VMEM((nz, group * tok, blk), bf16),
            pltpu.VMEM((ni, 2 * tok, half), bf16),
            pltpu.VMEM((3, blk, kv), bf16),
            pltpu.VMEM((2, blk, kv), bf16),
            pltpu.VMEM((2, blk, kv), jnp.float32),
            pltpu.VMEM((2, blk, kv), bf16),
            dma((4,)),
            dma, dma((2, 2)), dma((ni,)), dma,
            dma, dma((nz,)), dma, dma,
            dma, dma, dma((2, 2)),
            dma((2,)), dma((nz, 2)), dma, dma,
            *[pltpu.SemaphoreType.REGULAR] * 3,
        ],
        compiler_params=pltpu.CompilerParams(collective_id=0, has_side_effects=True),
    )(acts, grad_out, codes, scales.reshape(1, -1))
    return tuple(pl.pallas_call(
        leave,
        out_shape=(
            jax.ShapeDtypeStruct((tok, width), bf16),
            jax.ShapeDtypeStruct((blk, kv), jnp.float32),
        ),
        in_specs=[anyspace] * 2,
        out_specs=(anyspace,) * 2,
        scratch_shapes=[dma((2,))],
    )(*(pltpu.with_memory_space_constraint(x, pltpu.VMEM) for x in (gin, gw))))


def plain(acts, grad_out, codes, scales):
    rows = codes.shape[0]
    width_kv = codes.shape[1]
    blocks = codes.astype(jnp.float32).reshape(rows // 2, 2 * width_kv) * scales[:, None]
    local_weight = blocks.reshape(rows, width_kv).astype(jnp.bfloat16)
    n_group = lax.axis_size("intra")
    n_cross = lax.axis_size("inter")
    factor = 1.0 / math.sqrt(acts.shape[0] * n_group * n_cross)
    contract = (((0,), (0,)), ((), ()))
    group_cot = lax.all_gather(grad_out, "intra", axis=0, tiled=True)
    columns_owned = lax.all_to_all(acts, "intra", split_axis=1, concat_axis=0, tiled=True)
    grad_w = lax.psum_scatter(
        lax.dot_general(columns_owned, group_cot, contract, preferred_element_type=jnp.float32)
        * factor,
        "inter",
        scatter_dimension=0,
        tiled=True,
    )
    pieces = jnp.dot(group_cot, local_weight.T, preferred_element_type=jnp.float32).astype(
        jnp.bfloat16
    )
    grad_in = lax.all_to_all(pieces, "intra", split_axis=0, concat_axis=1, tiled=True)
    return (grad_in, grad_w)


def solution(mesh):
    ni, nj = mesh.shape["intra"], mesh.shape["inter"]

    def per_device(acts, grad_out, codes, scales):
        rows = codes.shape[0]
        aligned = rows % (nj * 128) == 0 and rows % 512 == 0 and acts.shape[0] % 16 == 0
        if aligned and nj == 8 and ni == 4 and acts.shape[1] == ni * rows:
            return fused(ni, nj, acts, grad_out, codes, scales)
        return plain(acts, grad_out, codes, scales)

    in_specs = (
        P(("intra", "inter"), None),
        P(("intra", "inter"), None),
        P("intra", None),
        P("intra"),
    )
    out_specs = (P(("intra", "inter"), None), P(("intra", "inter"), None))
    return jax.shard_map(
        per_device, mesh=mesh, in_specs=in_specs, out_specs=out_specs, check_vma=False
    )
```

```python
import functools
import math

import jax
import jax.numpy as jnp
from jax import lax
from jax.experimental import pallas as pl
from jax.experimental.pallas import tpu as pltpu
from jax.sharding import PartitionSpec as P

MESH = pl.DeviceIdType.MESH


def flip(index, mask, extent):
    out = 0
    bit = 1
    while bit < extent:
        digit = lax.rem(index // bit, 2)
        out = out + bit * (1 - digit if mask & bit else digit)
        bit *= 2
    return out


def lane_scale(scale_row, half):
    pick = (
        lax.broadcasted_iota(jnp.int32, (half // 2, half), 1) // 2
        == lax.broadcasted_iota(jnp.int32, (half // 2, half), 0)
    ).astype(jnp.float32).astype(jnp.bfloat16)
    rest = jnp.broadcast_to(scale_row, (16, half // 2))
    total = jnp.zeros((16, half), jnp.float32)
    for _ in range(3):
        top = rest.astype(jnp.bfloat16)
        total = total + jnp.dot(top, pick, preferred_element_type=jnp.float32)
        rest = rest - top.astype(jnp.float32)
    return total[0:1]


def kernel(
    ni, nj, acts, go, codes, scales, gin, gw,
    go_all, acts_v, codes_v, scale_v, code_b, code_d, scale_d, ac, pieces, part, rs, held, ms,
    load_sem, go_send, go_recv, pair_recv, gh_recv, a_send, a_recv, p_send, p_recv,
    r_send, r_recv, m_recv, w_send, w_recv, s_send, s_recv, near_sem, diag_sem, line_sem,
):
    tok, width = acts.shape
    rows = codes.shape[0]
    half = rows // 2
    nz = nj // 2
    blk = rows // nj
    i = lax.axis_index("intra")
    j = lax.axis_index("inter")
    z = j // 2
    c = lax.rem(j, 2)
    oc = 1 - c
    me = 2 * i + c
    peers = {d: flip(i, d, ni) for d in range(ni)}
    near, diag = (1, 2), 3
    dd = peers[diag]
    cores = (c, oc)
    pair = z // 2
    inner = lax.rem(z, 2) != pair
    mate = 2 * pair + 1 - lax.rem(z, 2)
    far_outer = 3 * (1 - pair)
    far_inner = 2 - pair
    swap = jnp.where(inner, mate - far_inner, 0)
    order = [far_outer, far_inner + swap, mate - swap, z]

    def dev(ii, zz, cc):
        return {"intra": ii, "inter": 2 * zz + cc}

    def rdma(src, dst, s, r, where):
        return pltpu.make_async_remote_copy(
            src_ref=src, dst_ref=dst, send_sem=s, recv_sem=r, device_id=where, device_id_type=MESH
        )

    def arrived(ref, r):
        rdma(ref, ref, r, r, dev(i, z, oc)).wait_recv()

    def drained(ref, s):
        rdma(ref, ref, s, s, dev(i, z, oc)).wait_send()

    def send(*args):
        rdma(*args).start()

    def go_slot(m):
        return go_all.at[pl.ds(pl.multiple_of(m * tok, tok), tok)]

    def go_half(m, n):
        return go_all.at[pl.ds(pl.multiple_of(m * tok + n * (tok // 2), tok // 2), tok // 2)]

    def ac_slot(h, m):
        return ac.at[h, pl.ds(pl.multiple_of(m * tok, tok), tok)]

    def cols_of(ii, cc):
        return pl.ds(pl.multiple_of(ii * rows + cc * half, half), half)

    share = [blk * n // 8 for n in (6, 9, 10, 7)]

    def shares(h, q):
        early = (share[h] // 2 + 15) // 16 * 16
        return pl.ds(sum(share[:h]) + q * early, share[h] - early if q else early)

    def by_plane(work):
        for k in range(nz):
            pl.when(z == k)(functools.partial(work, k))

    half_start = pl.multiple_of(c * half, half)
    sc_start = pl.multiple_of(c * (half // 2), half // 2)
    barrier = pltpu.get_barrier_semaphore()
    for d in near:
        pl.semaphore_signal(barrier, inc=1, device_id=dev(peers[d], z, 0), device_id_type=MESH)

    @pl.when(c == 1)
    def _():
        pl.semaphore_signal(barrier, inc=1, device_id=dev(i, z, 0), device_id_type=MESH)

    load_go = pltpu.make_async_copy(go, go_slot(me), load_sem.at[0])
    load_go.start()
    load_codes = pltpu.make_async_copy(codes.at[pl.ds(half_start, half)], codes_v, load_sem.at[2])
    load_codes.start()
    load_acts = pltpu.make_async_copy(acts, acts_v, load_sem.at[1])
    load_acts.start()
    load_scale = pltpu.make_async_copy(scales.at[:, pl.ds(sc_start, half // 2)], scale_v, load_sem.at[3])
    load_scale.start()
    for k in range(1, nz):
        pl.semaphore_signal(barrier, inc=1, device_id=dev(i, lax.rem(z + k, nz), 1), device_id_type=MESH)

    load_go.wait()

    @pl.when(c == 0)
    def _():
        pl.semaphore_wait(barrier, 2 * len(near) + 1)
        pl.semaphore_signal(near_sem, inc=1, device_id=dev(i, z, 1), device_id_type=MESH)

    @pl.when(c == 1)
    def _():
        pl.semaphore_wait(near_sem, 1)

    def send_go(late):
        for n, d in enumerate(near):
            part_go = go_half(me, 1 - n if late else n)
            send(part_go, part_go, go_send, go_recv.at[n, late], dev(peers[d], z, c))

    pl.semaphore_signal(diag_sem, inc=1, device_id=dev(peers[near[0]], z, c), device_id_type=MESH)
    send_go(0)
    send_go(1)
    send(go_slot(me), go_slot(me), go_send, pair_recv.at[0], dev(i, z, oc))

    load_codes.wait()
    code_b[...] = codes_v[...].astype(jnp.float32).astype(jnp.bfloat16)
    load_scale.wait()
    pl.semaphore_wait(diag_sem, 1)
    send(scale_v, scale_d, s_send, s_recv, dev(dd, z, c))
    row_scale = lane_scale(scale_v[...], half)

    @by_plane
    def _(k):
        for q in range(2):
            rows_q = shares(k, q)
            send(code_b.at[rows_q], code_d.at[rows_q], w_send.at[0], w_recv.at[k, q], dev(dd, z, c))


    load_acts.wait()

    def send_columns(n):
        h = order[n]
        for d in near + (0, diag):
            for k, cc in enumerate(cores):
                ii = peers[d]
                col = pl.multiple_of(ii * rows + (2 * h + cc) * blk, blk)
                if d or k:
                    send(acts_v.at[:, pl.ds(col, blk)], ac_slot(h, me), a_send, a_recv.at[n], dev(ii, z, cc))
                else:
                    ac_slot(h, me)[...] = acts_v[:, pl.ds(col, blk)]

    def wait_pair(d):
        arrived(go_slot(2 * peers[d] + oc), pair_recv.at[d])

    for n, d in enumerate(near):
        m = 2 * peers[d] + c
        arrived(go_half(m, n), go_recv.at[n, 0])
        send(go_half(m, n), go_half(m, n), go_send, gh_recv, dev(peers[diag ^ d], z, c))
    for n in range(nz):
        send_columns(n)

    @pl.when(c == 1)
    def _():
        pl.semaphore_wait(barrier, 2 * (nz - 1))
        pl.semaphore_signal(line_sem, inc=1, device_id=dev(i, z, 0), device_id_type=MESH)

    @pl.when(c == 0)
    def _():
        pl.semaphore_wait(line_sem, 1)

    def hop(n, h, q, to):
        rows_q = code_d.at[shares(h, q)]
        send(rows_q, rows_q, w_send.at[n], w_recv.at[h, q], dev(i, to, c))

    def landed(h, q):
        arrived(code_d.at[shares(h, q)], w_recv.at[h, q])

    @by_plane
    def _(k):
        for q in range(2):
            landed(k, q)
            hop(0, k, q, k ^ 1)
            if k in (1, 2):
                hop(1, k, q, 3 - k)

    for n, d in enumerate(near):
        m = 2 * peers[d] + c
        arrived(go_half(m, 1 - n), go_recv.at[n, 1])
        send(go_slot(m), go_slot(m), go_send, pair_recv.at[d], dev(i, z, oc))

    m = 2 * dd + c
    arrived(go_slot(m), gh_recv)
    send(go_slot(m), go_slot(m), go_send, pair_recv.at[diag], dev(i, z, oc))

    def pieces_of(ii, code, scale):
        pair = go_all[pl.ds(pl.multiple_of(2 * ii * tok, 2 * tok), 2 * tok)]
        out = lax.dot_general(
            pair, code[...], (((1,), (1,)), ((), ())), preferred_element_type=jnp.float32
        )
        return (out * scale).astype(jnp.bfloat16)

    def piece(n, cc):
        return pieces.at[n, pl.ds(pl.multiple_of(cc * tok, tok), tok)]

    def own_piece(n, ii):
        gin[:, cols_of(ii, c)] = piece(n, c)[...]
        send(piece(n, oc), gin.at[:, cols_of(ii, c)], p_send, p_recv, dev(i, z, oc))


    @by_plane
    def _(k):
        if k in (1, 2):
            for q in range(2):
                landed(k ^ 1, q)
                hop(1, k ^ 1, q, (3 - k) ^ 1)
            for q in range(2):
                hop(1, k ^ 1, q, 3 - k)
            for q in range(2):
                landed(3 - k, q)
                hop(2, 3 - k, q, k ^ 1)

    def term_of(n):
        h = order[n]
        arrived(ac.at[h, pl.ds(0, (2 * ni - 1) * tok)], a_recv.at[n])
        return lax.dot_general(
            ac[h], go_all[...], (((0,), (0,)), ((), ())), preferred_element_type=jnp.float32
        )

    def rows_of(q):
        return pl.ds(q * (blk // 2), blk // 2)

    def pass_on(n, q, dst, recv, to):
        send(part.at[n, rows_of(q)], dst.at[rows_of(q)], r_send, recv, dev(i, to, c))

    def give(n, term, dst, recv):
        part[n] = term.astype(jnp.bfloat16)
        for q in range(2):
            pass_on(n, q, dst, recv(q), mate)

    def split(n, on_inner, on_outer):
        term = term_of(n)
        pl.when(inner)(lambda: on_inner(term))
        pl.when(jnp.logical_not(inner))(lambda: on_outer(term))

    def hold(n):
        def keep(term):
            held[n] = term
        return keep

    def to_merge(n):
        return lambda term: give(n, term, ms.at[n], lambda q: m_recv.at[n, q])

    def to_mate(term):
        give(2, term, rs.at[0], lambda q: r_recv)

    def merge(n, to):
        for q in range(2):
            arrived(ms.at[n, rows_of(q)], m_recv.at[n, q])
            total = held[n, rows_of(q)] + ms[n, rows_of(q)].astype(jnp.float32)
            part[n, rows_of(q)] = total.astype(jnp.bfloat16)
            pass_on(n, q, rs.at[1], r_recv, to)

    for d in range(ni):
        wait_pair(d)
    split(0, hold(0), to_merge(0))

    for d in near:
        ii = peers[d]
        pieces[d] = pieces_of(ii, code_b, row_scale)
        for cc in cores:
            send(piece(d, cc), gin.at[:, cols_of(i, c)], p_send, p_recv, dev(ii, z, cc))
    pieces[0] = pieces_of(i, code_b, row_scale)
    own_piece(0, i)

    split(1, to_mate, to_merge(1))

    @pl.when(inner)
    def _():
        merge(0, far_outer)

    split(2, hold(1), to_mate)

    @pl.when(inner)
    def _():
        merge(1, far_inner)

    mine = term_of(3)

    @by_plane
    def _(k):
        left = ((3 - k) ^ 1,) if k in (1, 2) else (k ^ 1, (3 - k) ^ 1, 3 - k)
        for h in left:
            for q in range(2):
                landed(h, q)

    arrived(scale_d, s_recv)
    pieces[diag] = pieces_of(i, code_d, lane_scale(scale_d[...], half))
    own_piece(diag, dd)

    arrived(rs, r_recv)
    for n in range(2):
        mine = mine + rs[n].astype(jnp.float32)
    gw[...] = mine * (1.0 / math.sqrt(tok * ni * nj))

    drained(go_all.at[pl.ds(0, (2 * ni - 1) * tok)], go_send)
    drained(acts_v.at[:, pl.ds(0, nz * (2 * ni - 1) * blk)], a_send)
    drained(part, r_send)
    drained(scale_v, s_send)

    @by_plane
    def _(k):
        drained(code_d.at[pl.ds(0, 2 * share[k])], w_send.at[0])
        if k in (1, 2):
            drained(code_d.at[pl.ds(0, share[k] + 2 * share[k ^ 1])], w_send.at[1])
            drained(code_d.at[pl.ds(0, share[3 - k])], w_send.at[2])

    pieces_all = gin.at[:, pl.ds(0, 6 * half)]
    drained(pieces_all, p_send)
    arrived(pieces_all, p_recv)


def leave(gin, gw, gin_out, gw_out, sem):
    copies = [
        pltpu.make_async_copy(gin, gin_out, sem.at[0]),
        pltpu.make_async_copy(gw, gw_out, sem.at[1]),
    ]
    for cp in copies:
        cp.start()
    for cp in copies:
        cp.wait()


def fused(ni, nj, acts, grad_out, codes, scales):
    tok, width = acts.shape
    kv = grad_out.shape[1]
    rows = codes.shape[0]
    half, nz, blk = rows // 2, nj // 2, rows // nj
    group = 2 * ni
    dma = pltpu.SemaphoreType.DMA
    bf16 = jnp.bfloat16
    anyspace = pl.BlockSpec(memory_space=pl.ANY)
    gin, gw = pl.pallas_call(
        functools.partial(kernel, ni, nj),
        out_shape=(
            pltpu.VMEM((tok, width), bf16),
            pltpu.VMEM((blk, kv), jnp.float32),
        ),
        in_specs=[anyspace] * 4,
        out_specs=(pl.BlockSpec(memory_space=pltpu.VMEM),) * 2,
        scratch_shapes=[
            pltpu.VMEM((group * tok, kv), bf16),
            pltpu.VMEM((tok, width), bf16),
            pltpu.VMEM((half, kv), jnp.int32),
            pltpu.VMEM((1, half // 2), jnp.float32),
            pltpu.VMEM((half, kv), bf16),
            pltpu.VMEM((half, kv), bf16),
            pltpu.VMEM((1, half // 2), jnp.float32),
            pltpu.VMEM((nz, group * tok, blk), bf16),
            pltpu.VMEM((ni, 2 * tok, half), bf16),
            pltpu.VMEM((3, blk, kv), bf16),
            pltpu.VMEM((2, blk, kv), bf16),
            pltpu.VMEM((2, blk, kv), jnp.float32),
            pltpu.VMEM((2, blk, kv), bf16),
            dma((4,)),
            dma, dma((2, 2)), dma((ni,)), dma,
            dma, dma((nz,)), dma, dma,
            dma, dma, dma((2, 2)),
            dma((3,)), dma((nz, 2)), dma, dma,
            *[pltpu.SemaphoreType.REGULAR] * 3,
        ],
        compiler_params=pltpu.CompilerParams(collective_id=0, has_side_effects=True),
    )(acts, grad_out, codes, scales.reshape(1, -1))
    return tuple(pl.pallas_call(
        leave,
        out_shape=(
            jax.ShapeDtypeStruct((tok, width), bf16),
            jax.ShapeDtypeStruct((blk, kv), jnp.float32),
        ),
        in_specs=[anyspace] * 2,
        out_specs=(anyspace,) * 2,
        scratch_shapes=[dma((2,))],
    )(*(pltpu.with_memory_space_constraint(x, pltpu.VMEM) for x in (gin, gw))))


def plain(acts, grad_out, codes, scales):
    rows = codes.shape[0]
    width_kv = codes.shape[1]
    blocks = codes.astype(jnp.float32).reshape(rows // 2, 2 * width_kv) * scales[:, None]
    local_weight = blocks.reshape(rows, width_kv).astype(jnp.bfloat16)
    n_group = lax.axis_size("intra")
    n_cross = lax.axis_size("inter")
    factor = 1.0 / math.sqrt(acts.shape[0] * n_group * n_cross)
    contract = (((0,), (0,)), ((), ()))
    group_cot = lax.all_gather(grad_out, "intra", axis=0, tiled=True)
    columns_owned = lax.all_to_all(acts, "intra", split_axis=1, concat_axis=0, tiled=True)
    grad_w = lax.psum_scatter(
        lax.dot_general(columns_owned, group_cot, contract, preferred_element_type=jnp.float32)
        * factor,
        "inter",
        scatter_dimension=0,
        tiled=True,
    )
    pieces = jnp.dot(group_cot, local_weight.T, preferred_element_type=jnp.float32).astype(
        jnp.bfloat16
    )
    grad_in = lax.all_to_all(pieces, "intra", split_axis=0, concat_axis=1, tiled=True)
    return (grad_in, grad_w)


def solution(mesh):
    ni, nj = mesh.shape["intra"], mesh.shape["inter"]

    def per_device(acts, grad_out, codes, scales):
        rows = codes.shape[0]
        aligned = rows % (nj * 128) == 0 and rows % 512 == 0 and acts.shape[0] % 16 == 0
        if aligned and nj == 8 and ni == 4 and acts.shape[1] == ni * rows:
            return fused(ni, nj, acts, grad_out, codes, scales)
        return plain(acts, grad_out, codes, scales)

    in_specs = (
        P(("intra", "inter"), None),
        P(("intra", "inter"), None),
        P("intra", None),
        P("intra"),
    )
    out_specs = (P(("intra", "inter"), None), P(("intra", "inter"), None))
    return jax.shard_map(
        per_device, mesh=mesh, in_specs=in_specs, out_specs=out_specs, check_vma=False
    )
```

```python
import functools
import math

import jax
import jax.numpy as jnp
from jax import lax
from jax.experimental import pallas as pl
from jax.experimental.pallas import tpu as pltpu
from jax.sharding import PartitionSpec as P

MESH = pl.DeviceIdType.MESH


def flip(index, mask, extent):
    out = 0
    bit = 1
    while bit < extent:
        digit = lax.rem(index // bit, 2)
        out = out + bit * (1 - digit if mask & bit else digit)
        bit *= 2
    return out


def lane_scale(scale_row, half):
    pick = (
        lax.broadcasted_iota(jnp.int32, (half // 2, half), 1) // 2
        == lax.broadcasted_iota(jnp.int32, (half // 2, half), 0)
    ).astype(jnp.float32).astype(jnp.bfloat16)
    rest = jnp.broadcast_to(scale_row, (16, half // 2))
    total = jnp.zeros((16, half), jnp.float32)
    for _ in range(3):
        top = rest.astype(jnp.bfloat16)
        total = total + jnp.dot(top, pick, preferred_element_type=jnp.float32)
        rest = rest - top.astype(jnp.float32)
    return total[0:1]


def kernel(
    ni, nj, acts, go, codes, scales, gin, gw,
    go_all, acts_v, codes_v, scale_v, code_b, code_d, scale_d, ac, pieces, part, rs, held, ms,
    load_sem, go_send, go_recv, pair_recv, gh_recv, a_send, a_recv, p_send, p_recv,
    r_send, r_recv, m_recv, w_send, w_recv, s_send, s_recv, near_sem, diag_sem, line_sem,
):
    tok, width = acts.shape
    rows = codes.shape[0]
    half = rows // 2
    nz = nj // 2
    blk = rows // nj
    i = lax.axis_index("intra")
    j = lax.axis_index("inter")
    z = j // 2
    c = lax.rem(j, 2)
    oc = 1 - c
    me = 2 * i + c
    peers = {d: flip(i, d, ni) for d in range(ni)}
    near, diag = (1, 2), 3
    dd = peers[diag]
    cores = (c, oc)
    pair = z // 2
    inner = lax.rem(z, 2) != pair
    mate = 2 * pair + 1 - lax.rem(z, 2)
    far_outer = 3 * (1 - pair)
    far_inner = 2 - pair
    swap = jnp.where(inner, mate - far_inner, 0)
    order = [far_outer, far_inner + swap, mate - swap, z]

    def dev(ii, zz, cc):
        return {"intra": ii, "inter": 2 * zz + cc}

    def rdma(src, dst, s, r, where):
        return pltpu.make_async_remote_copy(
            src_ref=src, dst_ref=dst, send_sem=s, recv_sem=r, device_id=where, device_id_type=MESH
        )

    def arrived(ref, r):
        rdma(ref, ref, r, r, dev(i, z, oc)).wait_recv()

    def drained(ref, s):
        rdma(ref, ref, s, s, dev(i, z, oc)).wait_send()

    def send(*args):
        rdma(*args).start()

    def go_slot(m):
        return go_all.at[pl.ds(pl.multiple_of(m * tok, tok), tok)]

    def go_half(m, n):
        return go_all.at[pl.ds(pl.multiple_of(m * tok + n * (tok // 2), tok // 2), tok // 2)]

    def ac_slot(h, m):
        return ac.at[h, pl.ds(pl.multiple_of(m * tok, tok), tok)]

    def cols_of(ii, cc):
        return pl.ds(pl.multiple_of(ii * rows + cc * half, half), half)

    share = [blk * n // 8 for n in (6, 9, 10, 7)]

    def shares(h, q):
        early = (share[h] // 2 + 15) // 16 * 16
        return pl.ds(sum(share[:h]) + q * early, share[h] - early if q else early)

    def by_plane(work):
        for k in range(nz):
            pl.when(z == k)(functools.partial(work, k))

    half_start = pl.multiple_of(c * half, half)
    sc_start = pl.multiple_of(c * (half // 2), half // 2)
    barrier = pltpu.get_barrier_semaphore()
    for d in near:
        pl.semaphore_signal(barrier, inc=1, device_id=dev(peers[d], z, 1), device_id_type=MESH)

    @pl.when(c == 0)
    def _():
        pl.semaphore_signal(barrier, inc=1, device_id=dev(i, z, 1), device_id_type=MESH)

    load_go = pltpu.make_async_copy(go, go_slot(me), load_sem.at[0])
    load_go.start()
    load_codes = pltpu.make_async_copy(codes.at[pl.ds(half_start, half)], codes_v, load_sem.at[2])
    load_codes.start()
    load_acts = pltpu.make_async_copy(acts, acts_v, load_sem.at[1])
    load_acts.start()
    load_scale = pltpu.make_async_copy(scales.at[:, pl.ds(sc_start, half // 2)], scale_v, load_sem.at[3])
    load_scale.start()
    for k in range(1, nz):
        pl.semaphore_signal(barrier, inc=1, device_id=dev(i, lax.rem(z + k, nz), 0), device_id_type=MESH)

    load_go.wait()

    @pl.when(c == 1)
    def _():
        pl.semaphore_wait(barrier, 2 * len(near) + 1)
        pl.semaphore_signal(near_sem, inc=1, device_id=dev(i, z, 0), device_id_type=MESH)

    @pl.when(c == 0)
    def _():
        pl.semaphore_wait(near_sem, 1)

    def send_go(late):
        for n, d in enumerate(near):
            part_go = go_half(me, 1 - n if late else n)
            send(part_go, part_go, go_send, go_recv.at[n, late], dev(peers[d], z, c))

    pl.semaphore_signal(diag_sem, inc=1, device_id=dev(peers[near[0]], z, c), device_id_type=MESH)
    send_go(0)
    send_go(1)
    send(go_slot(me), go_slot(me), go_send, pair_recv.at[0], dev(i, z, oc))

    load_codes.wait()
    code_b[...] = codes_v[...].astype(jnp.float32).astype(jnp.bfloat16)
    load_scale.wait()
    pl.semaphore_wait(diag_sem, 1)
    send(scale_v, scale_d, s_send, s_recv, dev(dd, z, c))
    row_scale = lane_scale(scale_v[...], half)

    @by_plane
    def _(k):
        for q in range(2):
            rows_q = shares(k, q)
            send(code_b.at[rows_q], code_d.at[rows_q], w_send.at[0], w_recv.at[k, q], dev(dd, z, c))


    load_acts.wait()

    def send_columns(n):
        h = order[n]
        for d in near + (0, diag):
            for k, cc in enumerate(cores):
                ii = peers[d]
                col = pl.multiple_of(ii * rows + (2 * h + cc) * blk, blk)
                if d or k:
                    send(acts_v.at[:, pl.ds(col, blk)], ac_slot(h, me), a_send, a_recv.at[n], dev(ii, z, cc))
                else:
                    ac_slot(h, me)[...] = acts_v[:, pl.ds(col, blk)]

    def wait_pair(d):
        arrived(go_slot(2 * peers[d] + oc), pair_recv.at[d])

    for n, d in enumerate(near):
        m = 2 * peers[d] + c
        arrived(go_half(m, n), go_recv.at[n, 0])
        send(go_half(m, n), go_half(m, n), go_send, gh_recv, dev(peers[diag ^ d], z, c))
    for n in range(nz):
        send_columns(n)

    @pl.when(c == 0)
    def _():
        pl.semaphore_wait(barrier, 2 * (nz - 1))
        pl.semaphore_signal(line_sem, inc=1, device_id=dev(i, z, 1), device_id_type=MESH)

    @pl.when(c == 1)
    def _():
        pl.semaphore_wait(line_sem, 1)

    def hop(n, h, q, to):
        rows_q = code_d.at[shares(h, q)]
        send(rows_q, rows_q, w_send.at[n], w_recv.at[h, q], dev(i, to, c))

    def landed(h, q):
        arrived(code_d.at[shares(h, q)], w_recv.at[h, q])

    @by_plane
    def _(k):
        for q in range(2):
            landed(k, q)
            hop(0, k, q, k ^ 1)
            if k in (1, 2):
                hop(1, k, q, 3 - k)

    for n, d in enumerate(near):
        m = 2 * peers[d] + c
        arrived(go_half(m, 1 - n), go_recv.at[n, 1])
        send(go_slot(m), go_slot(m), go_send, pair_recv.at[d], dev(i, z, oc))

    m = 2 * dd + c
    arrived(go_slot(m), gh_recv)
    send(go_slot(m), go_slot(m), go_send, pair_recv.at[diag], dev(i, z, oc))

    def pieces_of(ii, code, scale):
        pair = go_all[pl.ds(pl.multiple_of(2 * ii * tok, 2 * tok), 2 * tok)]
        out = lax.dot_general(
            pair, code[...], (((1,), (1,)), ((), ())), preferred_element_type=jnp.float32
        )
        return (out * scale).astype(jnp.bfloat16)

    def piece(n, cc):
        return pieces.at[n, pl.ds(pl.multiple_of(cc * tok, tok), tok)]

    def own_piece(n, ii):
        gin[:, cols_of(ii, c)] = piece(n, c)[...]
        send(piece(n, oc), gin.at[:, cols_of(ii, c)], p_send, p_recv, dev(i, z, oc))


    @by_plane
    def _(k):
        if k in (1, 2):
            for q in range(2):
                landed(k ^ 1, q)
                hop(1, k ^ 1, q, (3 - k) ^ 1)
            for q in range(2):
                hop(1, k ^ 1, q, 3 - k)
            for q in range(2):
                landed(3 - k, q)
                hop(2, 3 - k, q, k ^ 1)

    def term_of(n):
        h = order[n]
        arrived(ac.at[h, pl.ds(0, (2 * ni - 1) * tok)], a_recv.at[n])
        return lax.dot_general(
            ac[h], go_all[...], (((0,), (0,)), ((), ())), preferred_element_type=jnp.float32
        )

    def rows_of(q):
        return pl.ds(q * (blk // 2), blk // 2)

    def pass_on(n, q, dst, recv, to):
        send(part.at[n, rows_of(q)], dst.at[rows_of(q)], r_send, recv, dev(i, to, c))

    def give(n, term, dst, recv):
        part[n] = term.astype(jnp.bfloat16)
        for q in range(2):
            pass_on(n, q, dst, recv(q), mate)

    def split(n, on_inner, on_outer):
        term = term_of(n)
        pl.when(inner)(lambda: on_inner(term))
        pl.when(jnp.logical_not(inner))(lambda: on_outer(term))

    def hold(n):
        def keep(term):
            held[n] = term
        return keep

    def to_merge(n):
        return lambda term: give(n, term, ms.at[n], lambda q: m_recv.at[n, q])

    def to_mate(term):
        give(2, term, rs.at[0], lambda q: r_recv)

    def merge(n, to):
        for q in range(2):
            arrived(ms.at[n, rows_of(q)], m_recv.at[n, q])
            total = held[n, rows_of(q)] + ms[n, rows_of(q)].astype(jnp.float32)
            part[n, rows_of(q)] = total.astype(jnp.bfloat16)
            pass_on(n, q, rs.at[1], r_recv, to)

    for d in range(ni):
        wait_pair(d)
    split(0, hold(0), to_merge(0))

    for d in near:
        ii = peers[d]
        pieces[d] = pieces_of(ii, code_b, row_scale)
        for cc in cores:
            send(piece(d, cc), gin.at[:, cols_of(i, c)], p_send, p_recv, dev(ii, z, cc))
    pieces[0] = pieces_of(i, code_b, row_scale)
    own_piece(0, i)

    split(1, to_mate, to_merge(1))

    @pl.when(inner)
    def _():
        merge(0, far_outer)

    split(2, hold(1), to_mate)

    @pl.when(inner)
    def _():
        merge(1, far_inner)

    mine = term_of(3)

    @by_plane
    def _(k):
        left = ((3 - k) ^ 1,) if k in (1, 2) else (k ^ 1, (3 - k) ^ 1, 3 - k)
        for h in left:
            for q in range(2):
                landed(h, q)

    arrived(scale_d, s_recv)
    pieces[diag] = pieces_of(i, code_d, lane_scale(scale_d[...], half))
    own_piece(diag, dd)

    arrived(rs, r_recv)
    for n in range(2):
        mine = mine + rs[n].astype(jnp.float32)
    gw[...] = mine * (1.0 / math.sqrt(tok * ni * nj))

    drained(go_all.at[pl.ds(0, (2 * ni - 1) * tok)], go_send)
    drained(acts_v.at[:, pl.ds(0, nz * (2 * ni - 1) * blk)], a_send)
    drained(part, r_send)
    drained(scale_v, s_send)

    @by_plane
    def _(k):
        drained(code_d.at[pl.ds(0, 2 * share[k])], w_send.at[0])
        if k in (1, 2):
            drained(code_d.at[pl.ds(0, share[k] + 2 * share[k ^ 1])], w_send.at[1])
            drained(code_d.at[pl.ds(0, share[3 - k])], w_send.at[2])

    pieces_all = gin.at[:, pl.ds(0, 6 * half)]
    drained(pieces_all, p_send)
    arrived(pieces_all, p_recv)


def leave(gin, gw, gin_out, gw_out, sem):
    copies = [
        pltpu.make_async_copy(gin, gin_out, sem.at[0]),
        pltpu.make_async_copy(gw, gw_out, sem.at[1]),
    ]
    for cp in copies:
        cp.start()
    for cp in copies:
        cp.wait()


def fused(ni, nj, acts, grad_out, codes, scales):
    tok, width = acts.shape
    kv = grad_out.shape[1]
    rows = codes.shape[0]
    half, nz, blk = rows // 2, nj // 2, rows // nj
    group = 2 * ni
    dma = pltpu.SemaphoreType.DMA
    bf16 = jnp.bfloat16
    anyspace = pl.BlockSpec(memory_space=pl.ANY)
    gin, gw = pl.pallas_call(
        functools.partial(kernel, ni, nj),
        out_shape=(
            pltpu.VMEM((tok, width), bf16),
            pltpu.VMEM((blk, kv), jnp.float32),
        ),
        in_specs=[anyspace] * 4,
        out_specs=(pl.BlockSpec(memory_space=pltpu.VMEM),) * 2,
        scratch_shapes=[
            pltpu.VMEM((group * tok, kv), bf16),
            pltpu.VMEM((tok, width), bf16),
            pltpu.VMEM((half, kv), jnp.int32),
            pltpu.VMEM((1, half // 2), jnp.float32),
            pltpu.VMEM((half, kv), bf16),
            pltpu.VMEM((half, kv), bf16),
            pltpu.VMEM((1, half // 2), jnp.float32),
            pltpu.VMEM((nz, group * tok, blk), bf16),
            pltpu.VMEM((ni, 2 * tok, half), bf16),
            pltpu.VMEM((3, blk, kv), bf16),
            pltpu.VMEM((2, blk, kv), bf16),
            pltpu.VMEM((2, blk, kv), jnp.float32),
            pltpu.VMEM((2, blk, kv), bf16),
            dma((4,)),
            dma, dma((2, 2)), dma((ni,)), dma,
            dma, dma((nz,)), dma, dma,
            dma, dma, dma((2, 2)),
            dma((3,)), dma((nz, 2)), dma, dma,
            *[pltpu.SemaphoreType.REGULAR] * 3,
        ],
        compiler_params=pltpu.CompilerParams(collective_id=0, has_side_effects=True),
    )(acts, grad_out, codes, scales.reshape(1, -1))
    return tuple(pl.pallas_call(
        leave,
        out_shape=(
            jax.ShapeDtypeStruct((tok, width), bf16),
            jax.ShapeDtypeStruct((blk, kv), jnp.float32),
        ),
        in_specs=[anyspace] * 2,
        out_specs=(anyspace,) * 2,
        scratch_shapes=[dma((2,))],
    )(*(pltpu.with_memory_space_constraint(x, pltpu.VMEM) for x in (gin, gw))))


def plain(acts, grad_out, codes, scales):
    rows = codes.shape[0]
    width_kv = codes.shape[1]
    blocks = codes.astype(jnp.float32).reshape(rows // 2, 2 * width_kv) * scales[:, None]
    local_weight = blocks.reshape(rows, width_kv).astype(jnp.bfloat16)
    n_group = lax.axis_size("intra")
    n_cross = lax.axis_size("inter")
    factor = 1.0 / math.sqrt(acts.shape[0] * n_group * n_cross)
    contract = (((0,), (0,)), ((), ()))
    group_cot = lax.all_gather(grad_out, "intra", axis=0, tiled=True)
    columns_owned = lax.all_to_all(acts, "intra", split_axis=1, concat_axis=0, tiled=True)
    grad_w = lax.psum_scatter(
        lax.dot_general(columns_owned, group_cot, contract, preferred_element_type=jnp.float32)
        * factor,
        "inter",
        scatter_dimension=0,
        tiled=True,
    )
    pieces = jnp.dot(group_cot, local_weight.T, preferred_element_type=jnp.float32).astype(
        jnp.bfloat16
    )
    grad_in = lax.all_to_all(pieces, "intra", split_axis=0, concat_axis=1, tiled=True)
    return (grad_in, grad_w)


def solution(mesh):
    ni, nj = mesh.shape["intra"], mesh.shape["inter"]

    def per_device(acts, grad_out, codes, scales):
        rows = codes.shape[0]
        aligned = rows % (nj * 128) == 0 and rows % 512 == 0 and acts.shape[0] % 16 == 0
        if aligned and nj == 8 and ni == 4 and acts.shape[1] == ni * rows:
            return fused(ni, nj, acts, grad_out, codes, scales)
        return plain(acts, grad_out, codes, scales)

    in_specs = (
        P(("intra", "inter"), None),
        P(("intra", "inter"), None),
        P("intra", None),
        P("intra"),
    )
    out_specs = (P(("intra", "inter"), None), P(("intra", "inter"), None))
    return jax.shard_map(
        per_device, mesh=mesh, in_specs=in_specs, out_specs=out_specs, check_vma=False
    )
```

```python
import functools
import math

import jax
import jax.numpy as jnp
from jax import lax
from jax.experimental import pallas as pl
from jax.experimental.pallas import tpu as pltpu
from jax.sharding import PartitionSpec as P

MESH = pl.DeviceIdType.MESH


def flip(index, mask, extent):
    out = 0
    bit = 1
    while bit < extent:
        digit = lax.rem(index // bit, 2)
        out = out + bit * (1 - digit if mask & bit else digit)
        bit *= 2
    return out


def lane_scale(scale_row, half):
    pick = (
        lax.broadcasted_iota(jnp.int32, (half // 2, half), 1) // 2
        == lax.broadcasted_iota(jnp.int32, (half // 2, half), 0)
    ).astype(jnp.float32).astype(jnp.bfloat16)
    rest = jnp.broadcast_to(scale_row, (16, half // 2))
    total = jnp.zeros((16, half), jnp.float32)
    for _ in range(3):
        top = rest.astype(jnp.bfloat16)
        total = total + jnp.dot(top, pick, preferred_element_type=jnp.float32)
        rest = rest - top.astype(jnp.float32)
    return total[0:1]


def kernel(
    ni, nj, acts, go, codes, scales, gin, gw,
    go_all, acts_v, codes_v, scale_v, code_b, code_d, scale_d, ac, pieces, part, rs, held, ms,
    load_sem, go_send, go_recv, pair_recv, gh_recv, a_send, a_recv, p_send, p_recv,
    r_send, r_recv, m_recv, w_send, w_recv, s_send, s_recv, near_sem, diag_sem, line_sem,
):
    tok, width = acts.shape
    rows = codes.shape[0]
    half = rows // 2
    nz = nj // 2
    blk = rows // nj
    i = lax.axis_index("intra")
    j = lax.axis_index("inter")
    z = j // 2
    c = lax.rem(j, 2)
    oc = 1 - c
    me = 2 * i + c
    peers = {d: flip(i, d, ni) for d in range(ni)}
    near, diag = (1, 2), 3
    dd = peers[diag]
    cores = (c, oc)
    pair = z // 2
    inner = lax.rem(z, 2) != pair
    mate = 2 * pair + 1 - lax.rem(z, 2)
    far_outer = 3 * (1 - pair)
    far_inner = 2 - pair
    swap = jnp.where(inner, mate - far_inner, 0)
    order = [far_outer, far_inner + swap, mate - swap, z]

    def dev(ii, zz, cc):
        return {"intra": ii, "inter": 2 * zz + cc}

    def rdma(src, dst, s, r, where):
        return pltpu.make_async_remote_copy(
            src_ref=src, dst_ref=dst, send_sem=s, recv_sem=r, device_id=where, device_id_type=MESH
        )

    def arrived(ref, r):
        rdma(ref, ref, r, r, dev(i, z, oc)).wait_recv()

    def drained(ref, s):
        rdma(ref, ref, s, s, dev(i, z, oc)).wait_send()

    def send(*args):
        rdma(*args).start()

    def go_slot(m):
        return go_all.at[pl.ds(pl.multiple_of(m * tok, tok), tok)]

    def go_half(m, n):
        return go_all.at[pl.ds(pl.multiple_of(m * tok + n * (tok // 2), tok // 2), tok // 2)]

    def ac_slot(h, m):
        return ac.at[h, pl.ds(pl.multiple_of(m * tok, tok), tok)]

    def cols_of(ii, cc):
        return pl.ds(pl.multiple_of(ii * rows + cc * half, half), half)

    share = [blk * n // 8 for n in (7, 9, 9, 7)]

    def shares(h, q):
        early = (share[h] // 2 + 15) // 16 * 16
        return pl.ds(sum(share[:h]) + q * early, share[h] - early if q else early)

    def by_plane(work):
        for k in range(nz):
            pl.when(z == k)(functools.partial(work, k))

    half_start = pl.multiple_of(c * half, half)
    sc_start = pl.multiple_of(c * (half // 2), half // 2)
    barrier = pltpu.get_barrier_semaphore()
    for d in near:
        pl.semaphore_signal(barrier, inc=1, device_id=dev(peers[d], z, 1), device_id_type=MESH)

    @pl.when(c == 0)
    def _():
        pl.semaphore_signal(barrier, inc=1, device_id=dev(i, z, 1), device_id_type=MESH)

    load_go = pltpu.make_async_copy(go, go_slot(me), load_sem.at[0])
    load_go.start()
    load_codes = pltpu.make_async_copy(codes.at[pl.ds(half_start, half)], codes_v, load_sem.at[2])
    load_codes.start()
    load_acts = pltpu.make_async_copy(acts, acts_v, load_sem.at[1])
    load_acts.start()
    load_scale = pltpu.make_async_copy(scales.at[:, pl.ds(sc_start, half // 2)], scale_v, load_sem.at[3])
    load_scale.start()
    for k in range(1, nz):
        pl.semaphore_signal(barrier, inc=1, device_id=dev(i, lax.rem(z + k, nz), 0), device_id_type=MESH)

    load_go.wait()

    @pl.when(c == 1)
    def _():
        pl.semaphore_wait(barrier, 2 * len(near) + 1)
        pl.semaphore_signal(near_sem, inc=1, device_id=dev(i, z, 0), device_id_type=MESH)

    @pl.when(c == 0)
    def _():
        pl.semaphore_wait(near_sem, 1)

    def send_go(late):
        for n, d in enumerate(near):
            part_go = go_half(me, 1 - n if late else n)
            send(part_go, part_go, go_send, go_recv.at[n, late], dev(peers[d], z, c))

    pl.semaphore_signal(diag_sem, inc=1, device_id=dev(peers[near[0]], z, c), device_id_type=MESH)
    send_go(0)
    send_go(1)
    send(go_slot(me), go_slot(me), go_send, pair_recv.at[0], dev(i, z, oc))

    load_codes.wait()
    code_b[...] = codes_v[...].astype(jnp.float32).astype(jnp.bfloat16)
    load_scale.wait()
    pl.semaphore_wait(diag_sem, 1)
    send(scale_v, scale_d, s_send, s_recv, dev(dd, z, c))
    row_scale = lane_scale(scale_v[...], half)

    @by_plane
    def _(k):
        for q in range(2):
            rows_q = shares(k, q)
            send(code_b.at[rows_q], code_d.at[rows_q], w_send.at[0], w_recv.at[k, q], dev(dd, z, c))


    load_acts.wait()

    def send_columns(n):
        h = order[n]
        for d in near + (0, diag):
            for k, cc in enumerate(cores):
                ii = peers[d]
                col = pl.multiple_of(ii * rows + (2 * h + cc) * blk, blk)
                if d or k:
                    send(acts_v.at[:, pl.ds(col, blk)], ac_slot(h, me), a_send, a_recv.at[n], dev(ii, z, cc))
                else:
                    ac_slot(h, me)[...] = acts_v[:, pl.ds(col, blk)]

    def wait_pair(d):
        arrived(go_slot(2 * peers[d] + oc), pair_recv.at[d])

    for n, d in enumerate(near):
        m = 2 * peers[d] + c
        arrived(go_half(m, n), go_recv.at[n, 0])
        send(go_half(m, n), go_half(m, n), go_send, gh_recv, dev(peers[diag ^ d], z, c))
    for n in range(nz):
        send_columns(n)

    @pl.when(c == 0)
    def _():
        pl.semaphore_wait(barrier, 2 * (nz - 1))
        pl.semaphore_signal(line_sem, inc=1, device_id=dev(i, z, 1), device_id_type=MESH)

    @pl.when(c == 1)
    def _():
        pl.semaphore_wait(line_sem, 1)

    def hop(n, h, q, to):
        rows_q = code_d.at[shares(h, q)]
        send(rows_q, rows_q, w_send.at[n], w_recv.at[h, q], dev(i, to, c))

    def landed(h, q):
        arrived(code_d.at[shares(h, q)], w_recv.at[h, q])

    @by_plane
    def _(k):
        for q in range(2):
            landed(k, q)
            hop(0, k, q, k ^ 1)
            if k in (1, 2):
                hop(1, k, q, 3 - k)

    for n, d in enumerate(near):
        m = 2 * peers[d] + c
        arrived(go_half(m, 1 - n), go_recv.at[n, 1])
        send(go_slot(m), go_slot(m), go_send, pair_recv.at[d], dev(i, z, oc))

    m = 2 * dd + c
    arrived(go_slot(m), gh_recv)
    send(go_slot(m), go_slot(m), go_send, pair_recv.at[diag], dev(i, z, oc))

    def pieces_of(ii, code, scale):
        pair = go_all[pl.ds(pl.multiple_of(2 * ii * tok, 2 * tok), 2 * tok)]
        out = lax.dot_general(
            pair, code[...], (((1,), (1,)), ((), ())), preferred_element_type=jnp.float32
        )
        return (out * scale).astype(jnp.bfloat16)

    def piece(n, cc):
        return pieces.at[n, pl.ds(pl.multiple_of(cc * tok, tok), tok)]

    def own_piece(n, ii):
        gin[:, cols_of(ii, c)] = piece(n, c)[...]
        send(piece(n, oc), gin.at[:, cols_of(ii, c)], p_send, p_recv, dev(i, z, oc))


    @by_plane
    def _(k):
        if k in (1, 2):
            for q in range(2):
                landed(k ^ 1, q)
                hop(1, k ^ 1, q, (3 - k) ^ 1)
            for q in range(2):
                hop(1, k ^ 1, q, 3 - k)
            for q in range(2):
                landed(3 - k, q)
                hop(2, 3 - k, q, k ^ 1)

    def term_of(n):
        h = order[n]
        arrived(ac.at[h, pl.ds(0, (2 * ni - 1) * tok)], a_recv.at[n])
        return lax.dot_general(
            ac[h], go_all[...], (((0,), (0,)), ((), ())), preferred_element_type=jnp.float32
        )

    def rows_of(q):
        return pl.ds(q * (blk // 2), blk // 2)

    def pass_on(n, q, dst, recv, to):
        send(part.at[n, rows_of(q)], dst.at[rows_of(q)], r_send, recv, dev(i, to, c))

    def give(n, term, dst, recv):
        part[n] = term.astype(jnp.bfloat16)
        for q in range(2):
            pass_on(n, q, dst, recv(q), mate)

    def split(n, on_inner, on_outer):
        term = term_of(n)
        pl.when(inner)(lambda: on_inner(term))
        pl.when(jnp.logical_not(inner))(lambda: on_outer(term))

    def hold(n):
        def keep(term):
            held[n] = term
        return keep

    def to_merge(n):
        return lambda term: give(n, term, ms.at[n], lambda q: m_recv.at[n, q])

    def to_mate(term):
        give(2, term, rs.at[0], lambda q: r_recv)

    def merge(n, to):
        for q in range(2):
            arrived(ms.at[n, rows_of(q)], m_recv.at[n, q])
            total = held[n, rows_of(q)] + ms[n, rows_of(q)].astype(jnp.float32)
            part[n, rows_of(q)] = total.astype(jnp.bfloat16)
            pass_on(n, q, rs.at[1], r_recv, to)

    for d in range(ni):
        wait_pair(d)
    split(0, hold(0), to_merge(0))

    for d in near:
        ii = peers[d]
        pieces[d] = pieces_of(ii, code_b, row_scale)
        for cc in cores:
            send(piece(d, cc), gin.at[:, cols_of(i, c)], p_send, p_recv, dev(ii, z, cc))
    pieces[0] = pieces_of(i, code_b, row_scale)
    own_piece(0, i)

    split(1, to_mate, to_merge(1))

    @pl.when(inner)
    def _():
        merge(0, far_outer)

    split(2, hold(1), to_mate)

    @pl.when(inner)
    def _():
        merge(1, far_inner)

    mine = term_of(3)

    @by_plane
    def _(k):
        left = ((3 - k) ^ 1,) if k in (1, 2) else (k ^ 1, (3 - k) ^ 1, 3 - k)
        for h in left:
            for q in range(2):
                landed(h, q)

    arrived(scale_d, s_recv)
    pieces[diag] = pieces_of(i, code_d, lane_scale(scale_d[...], half))
    own_piece(diag, dd)

    arrived(rs, r_recv)
    for n in range(2):
        mine = mine + rs[n].astype(jnp.float32)
    gw[...] = mine * (1.0 / math.sqrt(tok * ni * nj))

    drained(go_all.at[pl.ds(0, (2 * ni - 1) * tok)], go_send)
    drained(acts_v.at[:, pl.ds(0, nz * (2 * ni - 1) * blk)], a_send)
    drained(part, r_send)
    drained(scale_v, s_send)

    @by_plane
    def _(k):
        drained(code_d.at[pl.ds(0, 2 * share[k])], w_send.at[0])
        if k in (1, 2):
            drained(code_d.at[pl.ds(0, share[k] + 2 * share[k ^ 1])], w_send.at[1])
            drained(code_d.at[pl.ds(0, share[3 - k])], w_send.at[2])

    pieces_all = gin.at[:, pl.ds(0, 6 * half)]
    drained(pieces_all, p_send)
    arrived(pieces_all, p_recv)


def leave(gin, gw, gin_out, gw_out, sem):
    copies = [
        pltpu.make_async_copy(gin, gin_out, sem.at[0]),
        pltpu.make_async_copy(gw, gw_out, sem.at[1]),
    ]
    for cp in copies:
        cp.start()
    for cp in copies:
        cp.wait()


def fused(ni, nj, acts, grad_out, codes, scales):
    tok, width = acts.shape
    kv = grad_out.shape[1]
    rows = codes.shape[0]
    half, nz, blk = rows // 2, nj // 2, rows // nj
    group = 2 * ni
    dma = pltpu.SemaphoreType.DMA
    bf16 = jnp.bfloat16
    anyspace = pl.BlockSpec(memory_space=pl.ANY)
    gin, gw = pl.pallas_call(
        functools.partial(kernel, ni, nj),
        out_shape=(
            pltpu.VMEM((tok, width), bf16),
            pltpu.VMEM((blk, kv), jnp.float32),
        ),
        in_specs=[anyspace] * 4,
        out_specs=(pl.BlockSpec(memory_space=pltpu.VMEM),) * 2,
        scratch_shapes=[
            pltpu.VMEM((group * tok, kv), bf16),
            pltpu.VMEM((tok, width), bf16),
            pltpu.VMEM((half, kv), jnp.int32),
            pltpu.VMEM((1, half // 2), jnp.float32),
            pltpu.VMEM((half, kv), bf16),
            pltpu.VMEM((half, kv), bf16),
            pltpu.VMEM((1, half // 2), jnp.float32),
            pltpu.VMEM((nz, group * tok, blk), bf16),
            pltpu.VMEM((ni, 2 * tok, half), bf16),
            pltpu.VMEM((3, blk, kv), bf16),
            pltpu.VMEM((2, blk, kv), bf16),
            pltpu.VMEM((2, blk, kv), jnp.float32),
            pltpu.VMEM((2, blk, kv), bf16),
            dma((4,)),
            dma, dma((2, 2)), dma((ni,)), dma,
            dma, dma((nz,)), dma, dma,
            dma, dma, dma((2, 2)),
            dma((3,)), dma((nz, 2)), dma, dma,
            *[pltpu.SemaphoreType.REGULAR] * 3,
        ],
        compiler_params=pltpu.CompilerParams(collective_id=0, has_side_effects=True),
    )(acts, grad_out, codes, scales.reshape(1, -1))
    return tuple(pl.pallas_call(
        leave,
        out_shape=(
            jax.ShapeDtypeStruct((tok, width), bf16),
            jax.ShapeDtypeStruct((blk, kv), jnp.float32),
        ),
        in_specs=[anyspace] * 2,
        out_specs=(anyspace,) * 2,
        scratch_shapes=[dma((2,))],
    )(*(pltpu.with_memory_space_constraint(x, pltpu.VMEM) for x in (gin, gw))))


def plain(acts, grad_out, codes, scales):
    rows = codes.shape[0]
    width_kv = codes.shape[1]
    blocks = codes.astype(jnp.float32).reshape(rows // 2, 2 * width_kv) * scales[:, None]
    local_weight = blocks.reshape(rows, width_kv).astype(jnp.bfloat16)
    n_group = lax.axis_size("intra")
    n_cross = lax.axis_size("inter")
    factor = 1.0 / math.sqrt(acts.shape[0] * n_group * n_cross)
    contract = (((0,), (0,)), ((), ()))
    group_cot = lax.all_gather(grad_out, "intra", axis=0, tiled=True)
    columns_owned = lax.all_to_all(acts, "intra", split_axis=1, concat_axis=0, tiled=True)
    grad_w = lax.psum_scatter(
        lax.dot_general(columns_owned, group_cot, contract, preferred_element_type=jnp.float32)
        * factor,
        "inter",
        scatter_dimension=0,
        tiled=True,
    )
    pieces = jnp.dot(group_cot, local_weight.T, preferred_element_type=jnp.float32).astype(
        jnp.bfloat16
    )
    grad_in = lax.all_to_all(pieces, "intra", split_axis=0, concat_axis=1, tiled=True)
    return (grad_in, grad_w)


def solution(mesh):
    ni, nj = mesh.shape["intra"], mesh.shape["inter"]

    def per_device(acts, grad_out, codes, scales):
        rows = codes.shape[0]
        aligned = rows % (nj * 128) == 0 and rows % 512 == 0 and acts.shape[0] % 16 == 0
        if aligned and nj == 8 and ni == 4 and acts.shape[1] == ni * rows:
            return fused(ni, nj, acts, grad_out, codes, scales)
        return plain(acts, grad_out, codes, scales)

    in_specs = (
        P(("intra", "inter"), None),
        P(("intra", "inter"), None),
        P("intra", None),
        P("intra"),
    )
    out_specs = (P(("intra", "inter"), None), P(("intra", "inter"), None))
    return jax.shard_map(
        per_device, mesh=mesh, in_specs=in_specs, out_specs=out_specs, check_vma=False
    )
```
